256 devices in a mesh: slab: 64 (over z, y, core), pencil: 4 (over x).
Axes of the slice: x: 4, y: 4, z: 8, core: 2. Of those that a mesh axis runs over, the one named last changes fastest.
Arguments:
- density_history: float32 [7, 512, 320, 320], P(None, 'slab', 'pencil'), may hold values from -6 to 6
- residual_history: float32 [7, 512, 320, 320], P(None, 'slab', 'pencil'), as said below
- occupancy_history: float32 [7, 6144, 324], P(None, ('slab', 'pencil')), may hold values from -6 to 6
- occupancy_residual: float32 [7, 6144, 324], P(None, ('slab', 'pencil')), may hold values from -6 to 6
- species: int32 [6144], P(('slab', 'pencil')), may hold values from 0 to 3
- slot_count: int32 [256], P(('slab', 'pencil')), may hold values from 12 to 24, as said below
Outputs:
- new_density: float32 [512, 320, 320], P('slab', 'pencil')
- new_occupancy: float32 [6144, 324], P(('slab', 'pencil'))
The draws below stay inside these ranges and needn't reach their ends.
Inputs may be any that keep to these rules, and one draw needn't show every extreme that they name: `residual_history`: residual fields of the 7 previous steps. Device d of slab+pencil (slab slowest) holds slots d * 24 to (d + 1) * 24 - 1, of which the first slot_count[d] hold atoms; some device is full in every draw.
All inputs are finite; a program needn't handle non-finite values.
Results may differ from the reference program's by a relative error of at most 0.00017.
Values sent between devices are 32-bit elements; how exact they have to be, the bound alone decides.
No kernel may reach another device: no remote copies, remote signals or barrier semaphores. Data moves between devices by JAX's collectives and lax.ppermute only.
A program may use at most 128 MiB of HBM per device.

```python
import math
import jax
import jax.numpy as jnp
from jax import lax

HISTORY = 7
NX = 320
NY = 320
NZ = 512
ORBITALS = 18
SLOT_DEV = 24
SLOTS = 6144


def smooth_lines(key, leading, length):
    keys = jax.random.split(key, 2)
    amplitude = 0.5 * jax.random.normal(keys[0], leading + (4,), jnp.float32)
    phase = jax.random.uniform(keys[1], leading + (4,), jnp.float32, 0.0, 2.0 * math.pi)
    position = jnp.arange(length, dtype=jnp.float32)
    wavenumber = jnp.arange(1, 5, dtype=jnp.float32)
    angle = 2.0 * math.pi * wavenumber[:, None] * position[None, :] / length
    return jnp.sum(amplitude[..., None] * jnp.cos(angle + phase[..., None]), axis=-2)


def region_scale(key, length, upper):
    return jnp.exp(jax.random.uniform(key, (length,), jnp.float32, 0.0, math.log(upper)))


def draw_residual_history(key, part):
    keys = jax.random.split(key, 11)
    shared = 0.6
    spread = 4.0
    upper = 3.0
    common_noise = jax.random.normal(keys[0], (NZ, NY, NX), jnp.float32)
    own_noise = jax.random.normal(keys[1], (HISTORY, NZ, NY, NX), jnp.float32)
    region = region_scale(keys[2], NZ, upper)[:, None, None] * region_scale(keys[3], NY, upper)[None, :, None] * region_scale(keys[4], NX, upper)[None, None, :]
    common_smooth = smooth_lines(keys[5], (), NZ)[:, None, None] + smooth_lines(keys[6], (), NY)[None, :, None] + smooth_lines(keys[7], (), NX)[None, None, :]
    own_smooth = smooth_lines(keys[8], (HISTORY,), NZ)[:, :, None, None] + smooth_lines(keys[9], (HISTORY,), NY)[:, None, :, None] + smooth_lines(keys[10], (HISTORY,), NX)[:, None, None, :]
    common = common_noise * region + common_smooth
    own = own_noise * region[None] + own_smooth
    step_index = jnp.arange(HISTORY, dtype=jnp.float32)
    history_scale = jnp.exp(math.log(spread) * (1.0 - step_index / max(HISTORY - 1, 1)))
    value = history_scale[:, None, None, None] * (shared * common[None] + math.sqrt(1.0 - shared * shared) * own)
    return value.astype(jnp.float32)


def draw_slot_count(key, part):
    keys = jax.random.split(key, 2)
    devices_total = SLOTS // SLOT_DEV
    counts = jax.random.randint(keys[0], (devices_total,), max(1, SLOT_DEV // 2), SLOT_DEV + 1)
    filled = jax.random.randint(keys[1], (), 0, devices_total)
    position = jnp.arange(devices_total, dtype=jnp.int32)
    return jnp.where(position == filled, SLOT_DEV, counts).astype(jnp.int32)


def set_ends(result, stream_key, least, top_value):
    spot = [jax.random.randint(jax.random.fold_in(stream_key, axis), (), 0, length) for axis, length in enumerate(result.shape)]
    main_axis = result.shape.index(max(result.shape))
    next_to = spot[:main_axis] + [(spot[main_axis] + 1) % result.shape[main_axis]] + spot[main_axis + 1:]
    return result.at[tuple(spot)].set(least).at[tuple(next_to)].set(top_value)


def block_levels(key, shape, cuts, least, largest):
    gain = 1.0
    for axis_at, parts in cuts:
        draws = jax.random.uniform(jax.random.fold_in(jax.random.fold_in(key, 6), axis_at), (parts,), jnp.float32, least / len(cuts), largest / len(cuts))
        gain = gain * jnp.repeat(jnp.exp(draws), shape[axis_at] // parts).reshape((-1,) + (1,) * (len(shape) - 1 - axis_at))
    return gain


def gaussian(key, shape, width, reach, cuts=(), kind=jnp.bfloat16):
    drawn = jax.random.normal(key, shape, jnp.float32) * width
    if len(cuts) > 0:
        drawn = block_levels(key, shape, cuts, -0.22, 0.18) * drawn
    return jnp.clip(drawn, min=-reach, max=reach).astype(kind)


def setup_inputs(seed: int = 0) -> dict:
    key_of = jax.random.split(jax.random.key(seed), 7)
    return {
        "density_history": gaussian(key_of[0], (HISTORY, NZ, NY, NX), 1.0, 6.0, ((1, 64), (2, 4)), jnp.float32),
        "residual_history": draw_residual_history(jax.random.fold_in(key_of[6], 71), 0),
        "occupancy_history": gaussian(key_of[2], (HISTORY, SLOTS, ORBITALS * ORBITALS), 1.0, 6.0, ((1, 256),), jnp.float32),
        "occupancy_residual": gaussian(key_of[3], (HISTORY, SLOTS, ORBITALS * ORBITALS), 1.0, 6.0, ((1, 256),), jnp.float32),
        "species": set_ends(jax.random.randint(key_of[4], (SLOTS,), 0, 4), jax.random.fold_in(key_of[4], 1), 0, 3).astype(jnp.int32),
        "slot_count": draw_slot_count(jax.random.fold_in(key_of[6], 71), 0),
    }


highest = lax.Precision.HIGHEST
grid_mixing = 0.5
block_mixing = 0.5
kerker_wave = 6.0
species_orbitals = (18, 13, 8, 5)

def block_mask(species, slot_count):
    position = jnp.arange(species.shape[0], dtype=jnp.int32)
    owner_count = slot_count[(position // SLOT_DEV).astype(jnp.int32)]
    live = position % SLOT_DEV < owner_count
    orbitals = jnp.zeros_like(species)
    for species_index, orbital_number in enumerate(species_orbitals):
        orbitals = orbitals + orbital_number * (species == species_index).astype(jnp.int32)
    entry = jnp.arange(ORBITALS * ORBITALS, dtype=jnp.int32)
    row_index = entry // ORBITALS
    column_index = entry % ORBITALS
    inside = (row_index[None, :] < orbitals[:, None]) & (column_index[None, :] < orbitals[:, None]) & live[:, None]
    return inside.astype(jnp.float32)

def mixing_weights(intersection):
    factor = jnp.linalg.cholesky(intersection)
    column = jnp.ones((intersection.shape[0], 1), intersection.dtype)
    middle = lax.linalg.triangular_solve(factor, column, left_side=True, lower=True)
    solved = lax.linalg.triangular_solve(factor, middle, left_side=True, lower=True, transpose_a=True)
    return solved[:, 0] / jnp.sum(solved)

def magnitude(length):
    index = jnp.arange(length, dtype=jnp.int32)
    return jnp.minimum(index, length - index).astype(jnp.float32)

def reference(density_history, residual_history, occupancy_history, occupancy_residual, species, slot_count):
    mask = block_mask(species, slot_count)
    flat = residual_history.reshape(HISTORY, -1)
    grid_intersection = jnp.dot(flat, flat.T, precision=highest) / (NX * NY * NZ)
    blocks = (occupancy_residual * mask[None]).reshape(HISTORY, -1)
    block_intersection = jnp.dot(blocks, blocks.T, precision=highest) / (100.0 * SLOTS)
    weights = mixing_weights(grid_intersection + block_intersection)
    mixed = jnp.tensordot(weights, residual_history, axes=1, precision=highest)
    spectrum = jnp.fft.fftn(mixed)
    square = magnitude(NZ)[:, None, None] ** 2 + magnitude(NY)[None, :, None] ** 2 + magnitude(NX)[None, None, :] ** 2
    factor = square / (square + kerker_wave * kerker_wave)
    filtered = jnp.real(jnp.fft.ifftn(spectrum * factor)).astype(jnp.float32)
    new_density = jnp.tensordot(weights, density_history, axes=1, precision=highest) + grid_mixing * filtered
    mixed_blocks = jnp.tensordot(weights, occupancy_history + block_mixing * occupancy_residual, axes=1, precision=highest)
    return (new_density, mask * mixed_blocks)
```

```python
import functools
import math

import jax
import jax.numpy as jnp
import numpy as np
from jax import lax
from jax.experimental import pallas as pl
from jax.experimental.pallas import tpu as pltpu
from jax.sharding import Mesh
from jax.sharding import PartitionSpec as P

ORBITALS = 18
SLAB = ("slab_0", "slab_1", "slab_2")
SLAB_PENCIL = ("slab_0", "slab_1", "slab_2", "pencil")

grid_mixing = 0.5
block_mixing = 0.5
kerker_wave = 6.0
species_orbitals = (18, 13, 8, 5)

f32 = jnp.float32
bf16 = jnp.bfloat16
LANES = 128
MIB = 1 << 20


def pair_list(histories):
    return [(i, j) for i in range(histories) for j in range(i, histories)]


def split(value):
    high = value.astype(bf16)
    return high, (value - high.astype(f32)).astype(bf16)


def product(left, right, dims):
    dot = functools.partial(
        lax.dot_general, dimension_numbers=(dims, ((), ())), preferred_element_type=f32
    )
    return dot(left[0], right[0]) + (dot(left[0], right[1]) + dot(left[1], right[0]))


def hartley(rows, columns, length):
    angle = (np.outer(rows, columns) % length) * (2.0 * math.pi / length)
    table = np.cos(angle) + np.sin(angle)
    high = table.astype(bf16)
    low = (table - high.astype(np.float64)).astype(bf16)
    return high, low


def block_mask(species_ref, count_ref, slots, entries):
    row = lax.broadcasted_iota(jnp.int32, (slots, entries), 0)
    entry = lax.broadcasted_iota(jnp.int32, (slots, entries), 1)
    row_index = (entry * 3641) >> 16
    column_index = entry - ORBITALS * row_index
    limit = jnp.zeros((slots, entries), jnp.int32)
    for slot in range(slots):
        kind = species_ref[slot]
        number = jnp.int32(0)
        for index, orbital_number in enumerate(species_orbitals):
            number = jnp.where(kind == index, jnp.int32(orbital_number), number)
        number = jnp.where(slot < count_ref[0], number, jnp.int32(0))
        limit = jnp.where(row == slot, number, limit)
    return (row_index < limit) & (column_index < limit)


def gram_kernel(
    species_ref, count_ref, residual_ref, block_ref, out_ref, acc_ref, *, cell_total, block_total
):
    step = pl.program_id(0)
    histories, _, rows, width = residual_ref.shape
    pairs = pair_list(histories)

    @pl.when(step == 0)
    def _():
        acc_ref[...] = jnp.zeros_like(acc_ref)

    for start in range(0, width, LANES):
        lanes = slice(start, min(start + LANES, width))
        accs = [acc_ref[k, :, lanes] for k in range(len(pairs))]
        for top in range(0, rows, 8):
            values = [residual_ref[i, 0, top : top + 8, lanes] for i in range(histories)]
            accs = [acc + values[i] * values[j] for acc, (i, j) in zip(accs, pairs)]
        for k, acc in enumerate(accs):
            acc_ref[k, :, lanes] = acc

    @pl.when(step == pl.num_programs(0) - 1)
    def _():
        _, slots, entries = block_ref.shape
        mask = block_mask(species_ref, count_ref, slots, entries)
        blocks = [jnp.where(mask, block_ref[i], 0.0) for i in range(histories)]
        lane = lax.broadcasted_iota(jnp.int32, (1, LANES), 1)
        line = jnp.zeros((1, LANES), f32)
        for k, (i, j) in enumerate(pairs):
            grid_part = jnp.sum(acc_ref[k], axis=(0, 1), keepdims=True) / cell_total
            block_part = jnp.sum(blocks[i] * blocks[j], axis=(0, 1), keepdims=True) / block_total
            line = jnp.where(lane == k, grid_part + block_part, line)
        out_ref[...] = jnp.broadcast_to(line, out_ref.shape)


def mixing_weights(line, histories):
    lane = lax.broadcasted_iota(jnp.int32, (1, LANES), 1)
    entry = {}
    for k, (i, j) in enumerate(pair_list(histories)):
        entry[j, i] = jnp.sum(jnp.where(lane == k, line, 0.0), axis=1, keepdims=True)
    factor = {}
    inverse = {}
    work = dict(entry)
    for k in range(histories):
        inverse[k] = 1.0 / work[k, k]
        for i in range(k + 1, histories):
            factor[i, k] = work[i, k] * inverse[k]
        for i in range(k + 1, histories):
            for j in range(k + 1, i + 1):
                work[i, j] = work[i, j] - factor[i, k] * work[j, k]
    solved = [jnp.ones((1, 1), f32) for _ in range(histories)]
    for i in range(histories):
        for k in range(i):
            solved[i] = solved[i] - factor[i, k] * solved[k]
    solved = [value * inverse[i] for i, value in enumerate(solved)]
    for i in reversed(range(histories)):
        for k in range(i + 1, histories):
            solved[i] = solved[i] - factor[k, i] * solved[k]
    total = solved[0]
    for value in solved[1:]:
        total = total + value
    return [value / total for value in solved]


def mix_kernel(
    sums_ref, residual_ref, high_ref, low_ref, out_ref, weights_ref, mixed_high, mixed_low
):
    step = pl.program_id(0)
    histories, _, rows, width = residual_ref.shape

    @pl.when(step == 0)
    def _():
        line = jnp.sum(sums_ref[...], axis=0, keepdims=True)
        weights = mixing_weights(line, histories)
        for i, weight in enumerate(weights):
            weights_ref[i : i + 1, :] = jnp.broadcast_to(weight, (1, LANES))
        weights_ref[histories:, :] = jnp.zeros((8 - histories, LANES), f32)

    weights = [weights_ref[i : i + 1, 0:1] for i in range(histories)]
    mixed = weights[0] * residual_ref[0, 0]
    for i in range(1, histories):
        mixed = mixed + weights[i] * residual_ref[i, 0]
    high, low = split(mixed)
    mixed_high[pl.ds(step * rows, rows), :] = high
    mixed_low[pl.ds(step * rows, rows), :] = low

    @pl.when(step == pl.num_programs(0) - 1)
    def _():
        table = (high_ref[...], low_ref[...])
        result = product(table, (mixed_high[...], mixed_low[...]), ((1,), (1,)))
        pieces = result.shape[1] // LANES
        for piece in range(pieces):
            out_ref[pl.ds(piece, result.shape[0], stride=pieces), :] = result[
                :, piece * LANES : (piece + 1) * LANES
            ]


def z_forward_kernel(in_ref, high_ref, low_ref, out_ref, lines_ref, *, slab_count, z_local, y_local):
    z_length = slab_count * z_local
    per_slab = in_ref.shape[0] // slab_count
    pieces = z_local * y_local // LANES
    columns = per_slab // pieces
    for column in range(columns):
        turned = []
        for piece in range(pieces):
            block = in_ref[pl.ds(column * pieces + piece, slab_count, stride=per_slab), :]
            turned.append(block.T)
        turned = jnp.concatenate(turned, axis=0)
        lines_ref[column * y_local : (column + 1) * y_local, :] = jnp.concatenate(
            [turned[z * y_local : (z + 1) * y_local, :] for z in range(z_local)], axis=1
        )
    result = product(split(lines_ref[...]), (high_ref[...], low_ref[...]), ((1,), (0,)))
    for part in range(z_length // LANES):
        out_ref[part] = result[:, part * LANES : (part + 1) * LANES]


def filter_kernel(
    place_ref, in_ref, high_ref, low_ref, out_ref, *, kx_local, x_length, y_length, z_length, scale
):
    pencil_count, _, kz_local = in_ref.shape
    y_local = y_length // pencil_count
    table = (high_ref[...], low_ref[...])
    lines = jnp.concatenate(
        [
            jnp.concatenate(
                [in_ref[q, j * y_local : (j + 1) * y_local, :] for q in range(pencil_count)], axis=0
            )
            for j in range(kx_local)
        ],
        axis=1,
    )
    spectrum = product(table, split(lines), ((1,), (0,)))
    freq_y = lax.broadcasted_iota(jnp.int32, (y_length, kz_local), 0)
    freq_z = lax.broadcasted_iota(jnp.int32, (y_length, kz_local), 1) + place_ref[1] * kz_local
    mag_y = jnp.minimum(freq_y, y_length - freq_y).astype(f32)
    mag_z = jnp.minimum(freq_z, z_length - freq_z).astype(f32)
    plane = mag_y * mag_y + mag_z * mag_z
    kept = []
    for j in range(kx_local):
        freq_x = place_ref[0] * kx_local + j
        mag_x = jnp.minimum(freq_x, x_length - freq_x).astype(f32)
        square = plane + mag_x * mag_x
        factor = square / (square + kerker_wave * kerker_wave) * scale
        kept.append(spectrum[:, j * kz_local : (j + 1) * kz_local] * factor)
    result = product(table, split(jnp.concatenate(kept, axis=1)), ((1,), (0,)))
    for q in range(pencil_count):
        for j in range(kx_local):
            out_ref[q, j * y_local : (j + 1) * y_local, :] = result[
                q * y_local : (q + 1) * y_local, j * kz_local : (j + 1) * kz_local
            ]


def z_inverse_kernel(in_ref, high_ref, low_ref, out_ref, *, slab_count, z_local, y_local):
    parts = in_ref.shape[0]
    per_slab = out_ref.shape[0] // slab_count
    pieces = z_local * y_local // LANES
    columns = per_slab // pieces
    lines = jnp.concatenate([in_ref[part] for part in range(parts)], axis=1)
    result = product(split(lines), (high_ref[...], low_ref[...]), ((1,), (1,)))
    for column in range(columns):
        block = result[column * y_local : (column + 1) * y_local, :]
        stacked = jnp.concatenate(
            [block[:, z * slab_count : (z + 1) * slab_count] for z in range(z_local)], axis=0
        )
        for piece in range(pieces):
            out_ref[pl.ds(column * pieces + piece, slab_count, stride=per_slab), :] = stacked[
                piece * LANES : (piece + 1) * LANES, :
            ].T


def mean_kernel(
    species_ref, count_ref, weights_ref, density_ref, block_ref, block_residual_ref, out_ref, out_block_ref
):
    step = pl.program_id(0)
    histories = density_ref.shape[0]
    weights = [weights_ref[i : i + 1, 0:1] for i in range(histories)]
    mean = weights[0] * density_ref[0, 0]
    for i in range(1, histories):
        mean = mean + weights[i] * density_ref[i, 0]
    out_ref[0] = mean

    @pl.when(step == 0)
    def _():
        _, slots, entries = block_ref.shape
        mask = block_mask(species_ref, count_ref, slots, entries)
        total = weights[0] * (block_ref[0] + block_mixing * block_residual_ref[0])
        for i in range(1, histories):
            total = total + weights[i] * (block_ref[i] + block_mixing * block_residual_ref[i])
        out_block_ref[...] = jnp.where(mask, total, 0.0)


def x_inverse_kernel(in_ref, mean_ref, high_ref, low_ref, out_ref):
    z_local, y_local, x_length = mean_ref.shape
    table = (high_ref[...], low_ref[...])
    pieces = z_local * y_local // LANES
    fields = []
    for piece in range(pieces):
        block = in_ref[pl.ds(piece, x_length, stride=pieces), :]
        fields.append(product(split(block.T), table, ((1,), (0,))))
    field = jnp.concatenate(fields, axis=0)
    for z in range(z_local):
        out_ref[z] = mean_ref[z] + field[z * y_local : (z + 1) * y_local, :]


def whole():
    return pl.BlockSpec(memory_space=pltpu.VMEM)


def scalars():
    return pl.BlockSpec(memory_space=pltpu.SMEM)


def params(limit):
    return pltpu.CompilerParams(vmem_limit_bytes=limit * MIB)


def body(
    density_history, residual_history, occupancy_history, occupancy_residual, species, slot_count
):
    histories, z_local, y_local, x_length = residual_history.shape
    slab_count = lax.axis_size(SLAB)
    pencil_count = lax.axis_size("pencil")
    devices = slab_count * pencil_count
    y_length = y_local * pencil_count
    z_length = z_local * slab_count
    slots, entries = occupancy_residual.shape[1:]
    kx_local = x_length // slab_count
    kz_local = z_length // pencil_count
    lines = kx_local * y_local
    rows = z_local * y_local * x_length // LANES
    cell_total = float(z_length * y_length * x_length)
    x_table = hartley(np.arange(x_length), np.arange(x_length), x_length)
    y_table = hartley(np.arange(y_length), np.arange(y_length), y_length)
    z_order = (np.arange(slab_count)[None, :] * z_local + np.arange(z_local)[:, None]).reshape(-1)
    z_table = hartley(z_order, np.arange(z_length), z_length)

    plane_in = pl.BlockSpec((histories, 1, y_local, x_length), lambda z: (0, z, 0, 0))
    sums = pl.pallas_call(
        functools.partial(
            gram_kernel, cell_total=cell_total, block_total=100.0 * slots * devices
        ),
        grid=(z_local,),
        in_specs=[scalars(), scalars(), plane_in, whole()],
        out_specs=whole(),
        out_shape=jax.ShapeDtypeStruct((devices, LANES), f32),
        scratch_shapes=[pltpu.VMEM((len(pair_list(histories)), 8, x_length), f32)],
        compiler_params=params(16),
        name="gram",
    )(species, slot_count, residual_history, occupancy_residual)
    sums = lax.all_to_all(
        sums.reshape(devices, 1, LANES), SLAB_PENCIL, split_axis=0, concat_axis=0, tiled=True
    ).reshape(devices, LANES)

    packed, weights = pl.pallas_call(
        mix_kernel,
        grid=(z_local,),
        in_specs=[whole(), plane_in, whole(), whole()],
        out_specs=[whole(), whole()],
        out_shape=[
            jax.ShapeDtypeStruct((rows, LANES), f32),
            jax.ShapeDtypeStruct((8, LANES), f32),
        ],
        scratch_shapes=[
            pltpu.VMEM((z_local * y_local, x_length), bf16),
            pltpu.VMEM((z_local * y_local, x_length), bf16),
        ],
        compiler_params=params(24),
        name="mix",
    )(sums, residual_history, *x_table)

    def slab_move(array):
        shape = (slab_count, rows // slab_count, 1, LANES)
        return lax.all_to_all(
            array.reshape(shape), SLAB, split_axis=0, concat_axis=0, tiled=True
        ).reshape(rows, LANES)

    def pencil_move(array):
        return lax.all_to_all(array, "pencil", split_axis=0, concat_axis=0, tiled=True)

    sizes = dict(slab_count=slab_count, z_local=z_local, y_local=y_local)
    moved = slab_move(packed)
    mean, new_occupancy = pl.pallas_call(
        mean_kernel,
        grid=(z_local,),
        in_specs=[scalars(), scalars(), whole(), plane_in, whole(), whole()],
        out_specs=[pl.BlockSpec((1, y_local, x_length), lambda z: (z, 0, 0)), whole()],
        out_shape=[
            jax.ShapeDtypeStruct((z_local, y_local, x_length), f32),
            jax.ShapeDtypeStruct((slots, entries), f32),
        ],
        compiler_params=params(16),
        name="mean",
    )(species, slot_count, weights, density_history, occupancy_history, occupancy_residual)
    spectrum = pl.pallas_call(
        functools.partial(z_forward_kernel, **sizes),
        in_specs=[whole()] * 3,
        out_specs=whole(),
        out_shape=jax.ShapeDtypeStruct((pencil_count, lines, kz_local), f32),
        scratch_shapes=[pltpu.VMEM((lines, z_length), f32)],
        compiler_params=params(24),
        name="z_forward",
    )(moved, *z_table)
    moved = pencil_move(spectrum)
    place = jnp.stack([lax.axis_index(SLAB), lax.axis_index("pencil")]).astype(jnp.int32)
    kept = pl.pallas_call(
        functools.partial(
            filter_kernel,
            kx_local=kx_local,
            x_length=x_length,
            y_length=y_length,
            z_length=z_length,
            scale=grid_mixing / cell_total,
        ),
        in_specs=[scalars(), whole(), whole(), whole()],
        out_specs=whole(),
        out_shape=jax.ShapeDtypeStruct((pencil_count, lines, kz_local), f32),
        compiler_params=params(24),
        name="filter",
    )(place, moved, *y_table)
    moved = pencil_move(kept)
    packed = pl.pallas_call(
        functools.partial(z_inverse_kernel, **sizes),
        in_specs=[whole()] * 3,
        out_specs=whole(),
        out_shape=jax.ShapeDtypeStruct((rows, LANES), f32),
        compiler_params=params(24),
        name="z_inverse",
    )(moved, *z_table)
    moved = slab_move(packed)
    new_density = pl.pallas_call(
        x_inverse_kernel,
        in_specs=[whole()] * 4,
        out_specs=whole(),
        out_shape=jax.ShapeDtypeStruct((z_local, y_local, x_length), f32),
        compiler_params=params(24),
        name="x_inverse",
    )(moved, mean, *x_table)
    return (new_density, new_occupancy)


def solution(mesh):
    torus = Mesh(
        mesh.devices.reshape(8, 4, 2, mesh.shape["pencil"]),
        ("slab_0", "slab_1", "slab_2", "pencil"),
    )
    placed = (
        P(None, SLAB, "pencil", None),
        P(None, SLAB, "pencil", None),
        P(None, SLAB_PENCIL, None),
        P(None, SLAB_PENCIL, None),
        P(SLAB_PENCIL),
        P(SLAB_PENCIL),
    )
    return jax.shard_map(
        body,
        mesh=torus,
        in_specs=placed,
        out_specs=(P(SLAB, "pencil", None), P(SLAB_PENCIL, None)),
        check_vma=False,
    )
```

```python
import functools
import math

import jax
import jax.numpy as jnp
import numpy as np
from jax import lax
from jax.experimental import pallas as pl
from jax.experimental.pallas import tpu as pltpu
from jax.sharding import Mesh
from jax.sharding import PartitionSpec as P

ORBITALS = 18
SLAB = ("slab_0", "slab_1", "slab_2")
SLAB_PENCIL = ("slab_0", "slab_1", "slab_2", "pencil")

grid_mixing = 0.5
block_mixing = 0.5
kerker_wave = 6.0
species_orbitals = (18, 13, 8, 5)

f32 = jnp.float32
bf16 = jnp.bfloat16
LANES = 128
MIB = 1 << 20


def pair_list(histories):
    return [(i, j) for i in range(histories) for j in range(i, histories)]


def split(value):
    high = value.astype(bf16)
    return high, (value - high.astype(f32)).astype(bf16)


def product(left, right, dims):
    dot = functools.partial(
        lax.dot_general, dimension_numbers=(dims, ((), ())), preferred_element_type=f32
    )
    return dot(left[0], right[0]) + (dot(left[0], right[1]) + dot(left[1], right[0]))


def hartley(rows, columns, length):
    angle = (np.outer(rows, columns) % length) * (2.0 * math.pi / length)
    table = np.cos(angle) + np.sin(angle)
    high = table.astype(bf16)
    low = (table - high.astype(np.float64)).astype(bf16)
    return high, low


def block_mask(species_ref, count_ref, slots, entries):
    row = lax.broadcasted_iota(jnp.int32, (slots, entries), 0)
    entry = lax.broadcasted_iota(jnp.int32, (slots, entries), 1)
    row_index = (entry * 3641) >> 16
    column_index = entry - ORBITALS * row_index
    limit = jnp.zeros((slots, entries), jnp.int32)
    for slot in range(slots):
        kind = species_ref[slot]
        number = jnp.int32(0)
        for index, orbital_number in enumerate(species_orbitals):
            number = jnp.where(kind == index, jnp.int32(orbital_number), number)
        number = jnp.where(slot < count_ref[0], number, jnp.int32(0))
        limit = jnp.where(row == slot, number, limit)
    return (row_index < limit) & (column_index < limit)


def gram_kernel(
    species_ref,
    count_ref,
    residual_ref,
    block_ref,
    out_ref,
    held_ref,
    acc_ref,
    arrived,
    *,
    cell_total,
    block_total,
):
    histories, planes, rows, width = residual_ref.shape
    pairs = pair_list(histories)

    def fetch(z):
        return pltpu.make_async_copy(residual_ref.at[:, z], held_ref.at[:, z], arrived.at[z])

    for z in range(planes):
        fetch(z).start()
    acc_ref[...] = jnp.zeros_like(acc_ref)
    _, slots, entries = block_ref.shape
    mask = block_mask(species_ref, count_ref, slots, entries)
    blocks = [jnp.where(mask, block_ref[i], 0.0) for i in range(histories)]
    lane = lax.broadcasted_iota(jnp.int32, (1, LANES), 1)
    line = jnp.zeros((1, LANES), f32)
    for k, (i, j) in enumerate(pairs):
        block_part = jnp.sum(blocks[i] * blocks[j], axis=(0, 1), keepdims=True) / block_total
        line = jnp.where(lane == k, block_part, line)

    def plane(z, carry):
        fetch(z).wait()
        for start in range(0, width, LANES):
            lanes = slice(start, min(start + LANES, width))
            accs = [acc_ref[k, :, lanes] for k in range(len(pairs))]
            for top in range(0, rows, 8):
                values = [held_ref[i, z, top : top + 8, lanes] for i in range(histories)]
                accs = [acc + values[i] * values[j] for acc, (i, j) in zip(accs, pairs)]
            for k, acc in enumerate(accs):
                acc_ref[k, :, lanes] = acc
        return carry

    lax.fori_loop(0, planes, plane, 0)
    for k in range(len(pairs)):
        grid_part = jnp.sum(acc_ref[k], axis=(0, 1), keepdims=True) / cell_total
        line = jnp.where(lane == k, line + grid_part, line)
    out_ref[...] = jnp.broadcast_to(line, out_ref.shape)


def mixing_weights(line, histories):
    lane = lax.broadcasted_iota(jnp.int32, (1, LANES), 1)
    entry = {}
    for k, (i, j) in enumerate(pair_list(histories)):
        entry[j, i] = jnp.sum(jnp.where(lane == k, line, 0.0), axis=1, keepdims=True)
    factor = {}
    inverse = {}
    work = dict(entry)
    for k in range(histories):
        inverse[k] = 1.0 / work[k, k]
        for i in range(k + 1, histories):
            factor[i, k] = work[i, k] * inverse[k]
        for i in range(k + 1, histories):
            for j in range(k + 1, i + 1):
                work[i, j] = work[i, j] - factor[i, k] * work[j, k]
    solved = [jnp.ones((1, 1), f32) for _ in range(histories)]
    for i in range(histories):
        for k in range(i):
            solved[i] = solved[i] - factor[i, k] * solved[k]
    solved = [value * inverse[i] for i, value in enumerate(solved)]
    for i in reversed(range(histories)):
        for k in range(i + 1, histories):
            solved[i] = solved[i] - factor[k, i] * solved[k]
    total = solved[0]
    for value in solved[1:]:
        total = total + value
    return [value / total for value in solved]


def mix_kernel(
    sums_ref, residual_ref, high_ref, low_ref, out_ref, weights_ref, mixed_high, mixed_low, *, slab_count
):
    histories, planes, rows, _ = residual_ref.shape
    line = jnp.sum(sums_ref[...], axis=0, keepdims=True)
    weights = mixing_weights(line, histories)
    for i, weight in enumerate(weights):
        weights_ref[i : i + 1, :] = jnp.broadcast_to(weight, (1, LANES))
    weights_ref[histories:, :] = jnp.zeros((8 - histories, LANES), f32)
    for z in range(planes):
        mixed = weights[0] * residual_ref[0, z]
        for i in range(1, histories):
            mixed = mixed + weights[i] * residual_ref[i, z]
        high, low = split(mixed)
        mixed_high[z * rows : (z + 1) * rows, :] = high
        mixed_low[z * rows : (z + 1) * rows, :] = low
    table = (high_ref[...], low_ref[...])
    result = product(table, (mixed_high[...], mixed_low[...]), ((1,), (1,)))
    pieces = result.shape[1] // LANES
    own_planes = result.shape[0] // slab_count - 1
    message = out_ref.shape[0] // (slab_count * own_planes)
    period = own_planes * message
    extra = message - pieces

    def put(row, plane, piece):
        out_ref[pl.ds(row, slab_count, stride=period), :] = result[
            plane * slab_count : (plane + 1) * slab_count, piece * LANES : (piece + 1) * LANES
        ]

    for own in range(own_planes):
        for piece in range(pieces):
            put(own * message + piece, own, piece)
        first = (pieces - extra) * (own // 2)
        for piece in range(extra):
            put(own * message + pieces + piece, own_planes, first + piece)


def plane_kernel(
    place_ref,
    in_ref,
    zh_ref,
    zl_ref,
    yh_ref,
    yl_ref,
    out_ref,
    main_ref,
    half_ref,
    *,
    slab_count,
    pencil_count,
    z_local,
    y_local,
    x_length,
    scale,
):
    z_length = slab_count * z_local
    y_length = pencil_count * y_local
    message = in_ref.shape[0] // (slab_count * pencil_count)
    period = pencil_count * message
    pieces = z_local * y_local // LANES
    extra = message - pieces
    half = z_local // 2
    half_rows = half * y_local
    spare = pieces * LANES - half_rows - (pieces - extra) * LANES
    in_half = place_ref[1] // 2
    out_half = place_ref[1] % 2

    def taken(row):
        return in_ref[pl.ds(row, slab_count, stride=period), :].T

    def spread(rows, count):
        return jnp.concatenate([rows[z * y_local : (z + 1) * y_local] for z in range(count)], axis=1)

    def stacked(block, count):
        return jnp.concatenate(
            [block[:, z * slab_count : (z + 1) * slab_count] for z in range(count)], axis=0
        )

    for q in range(pencil_count):
        here = slice(q * y_local, (q + 1) * y_local)
        rows = jnp.concatenate([taken(q * message + k) for k in range(pieces)], axis=0)
        main_ref[here, :] = spread(rows, z_local)
        rows = jnp.concatenate([taken(q * message + pieces + k) for k in range(extra)], axis=0)
        rows = jnp.where(in_half == 0, rows[:half_rows], rows[spare : spare + half_rows])
        half_ref[here, :] = spread(rows, half)

    z_table = (zh_ref[...], zl_ref[...])
    y_table = (yh_ref[...], yl_ref[...])

    def half_table(which):
        rows = pl.ds(pl.multiple_of(which * (z_length // 2), LANES), z_length // 2)
        return (zh_ref[rows, :], zl_ref[rows, :])

    lines = jnp.concatenate(
        [
            product(split(main_ref[...]), z_table, ((1,), (0,))),
            product(split(half_ref[...]), half_table(in_half), ((1,), (0,))),
        ],
        axis=1,
    )
    spectrum = product(y_table, split(lines), ((1,), (0,)))
    freq_y = lax.broadcasted_iota(jnp.int32, (y_length, z_length), 0)
    freq_z = lax.broadcasted_iota(jnp.int32, (y_length, z_length), 1)
    mag_y = jnp.minimum(freq_y, y_length - freq_y).astype(f32)
    mag_z = jnp.minimum(freq_z, z_length - freq_z).astype(f32)
    plane = mag_y * mag_y + mag_z * mag_z
    kept = []
    for j, own in enumerate((place_ref[1], pencil_count)):
        freq_x = place_ref[0] * (pencil_count + 1) + own
        mag_x = jnp.minimum(freq_x, x_length - freq_x).astype(f32)
        square = plane + mag_x * mag_x
        factor = square / (square + kerker_wave * kerker_wave) * scale
        kept.append(spectrum[:, j * z_length : (j + 1) * z_length] * factor)
    kept = product(y_table, split(jnp.concatenate(kept, axis=1)), ((1,), (0,)))
    main = product(split(kept[:, :z_length]), z_table, ((1,), (1,)))
    part = product(split(kept[:, z_length:]), half_table(out_half), ((1,), (1,)))
    filler = jnp.zeros((extra * LANES - half_rows, slab_count), f32)
    for q in range(pencil_count):
        here = slice(q * y_local, (q + 1) * y_local)
        rows = jnp.concatenate([stacked(main[here], z_local), stacked(part[here], half), filler], axis=0)
        for k in range(message):
            out_ref[pl.ds(q * message + k, slab_count, stride=period), :] = rows[
                k * LANES : (k + 1) * LANES
            ].T


def mean_kernel(
    species_ref, count_ref, weights_ref, density_ref, block_ref, block_residual_ref, out_ref, out_block_ref
):
    step = pl.program_id(0)
    histories = density_ref.shape[0]
    weights = [weights_ref[i : i + 1, 0:1] for i in range(histories)]
    mean = weights[0] * density_ref[0, 0]
    for i in range(1, histories):
        mean = mean + weights[i] * density_ref[i, 0]
    out_ref[0] = mean

    @pl.when(step == 0)
    def _():
        _, slots, entries = block_ref.shape
        mask = block_mask(species_ref, count_ref, slots, entries)
        total = weights[0] * (block_ref[0] + block_mixing * block_residual_ref[0])
        for i in range(1, histories):
            total = total + weights[i] * (block_ref[i] + block_mixing * block_residual_ref[i])
        out_block_ref[...] = jnp.where(mask, total, 0.0)


def x_inverse_kernel(
    in_ref, mean_ref, high_ref, low_ref, out_ref, field_ref, sent, *, slab_count, pencil_count
):
    rows, x_length = mean_ref.shape
    table = (high_ref[...], low_ref[...])
    pieces = rows // LANES
    message = in_ref.shape[0] // (slab_count * pencil_count)

    def taken(row):
        return in_ref[pl.ds(row, slab_count, stride=pencil_count * message), :]

    halves = []
    for out_half in range(2):
        parts = [
            taken(out_half * message + k) + taken((out_half + 2) * message + k)
            for k in range(pieces, message)
        ]
        halves.append(jnp.concatenate(parts, axis=1)[:, : rows // 2])
    shared = jnp.concatenate(halves, axis=1)

    def send(piece):
        here = pl.ds(piece * LANES, LANES)
        return pltpu.make_async_copy(field_ref.at[here], out_ref.at[here], sent.at[piece])

    for piece in range(pieces):
        here = slice(piece * LANES, (piece + 1) * LANES)
        block = [taken(q * message + piece) for q in range(pencil_count)]
        block.append(shared[:, here])
        field = product(split(jnp.concatenate(block, axis=0).T), table, ((1,), (0,)))
        field_ref[here, :] = mean_ref[here, :] + field
        send(piece).start()
    for piece in range(pieces):
        send(piece).wait()


def whole():
    return pl.BlockSpec(memory_space=pltpu.VMEM)


def scalars():
    return pl.BlockSpec(memory_space=pltpu.SMEM)


def in_hbm(array):
    return pltpu.with_memory_space_constraint(array, pltpu.HBM)


def params(limit):
    return pltpu.CompilerParams(vmem_limit_bytes=limit * MIB)


def body(
    density_history, residual_history, occupancy_history, occupancy_residual, species, slot_count
):
    histories, z_local, y_local, x_length = residual_history.shape
    slab_count = lax.axis_size(SLAB)
    pencil_count = lax.axis_size("pencil")
    devices = slab_count * pencil_count
    y_length = y_local * pencil_count
    z_length = z_local * slab_count
    slots, entries = occupancy_residual.shape[1:]
    kx_local = x_length // slab_count
    message = z_local * y_local // LANES + -(-z_local * y_local // (2 * LANES))
    rows = devices * message
    cell_total = float(z_length * y_length * x_length)
    x_order = (np.arange(slab_count)[None, :] * kx_local + np.arange(kx_local)[:, None]).reshape(-1)
    x_table = hartley(x_order, np.arange(x_length), x_length)
    y_table = hartley(np.arange(y_length), np.arange(y_length), y_length)
    z_order = (np.arange(slab_count)[None, :] * z_local + np.arange(z_local)[:, None]).reshape(-1)
    z_table = hartley(z_order, np.arange(z_length), z_length)
    place = jnp.stack([lax.axis_index(SLAB), lax.axis_index("pencil")]).astype(jnp.int32)
    place, species = lax.optimization_barrier((place, species))

    sums, held = pl.pallas_call(
        functools.partial(
            gram_kernel, cell_total=cell_total, block_total=100.0 * slots * devices
        ),
        in_specs=[scalars(), scalars(), pl.BlockSpec(memory_space=pltpu.HBM), whole()],
        out_specs=[whole(), whole()],
        out_shape=[
            jax.ShapeDtypeStruct((devices, LANES), f32),
            jax.ShapeDtypeStruct(residual_history.shape, f32),
        ],
        scratch_shapes=[
            pltpu.VMEM((len(pair_list(histories)), 8, x_length), f32),
            pltpu.SemaphoreType.DMA((z_local,)),
        ],
        compiler_params=params(16),
        name="gram",
    )(in_hbm(species), slot_count, in_hbm(residual_history), in_hbm(occupancy_residual))

    def exchange(array):
        return lax.all_to_all(
            array.reshape(devices, -1, 1, LANES), SLAB_PENCIL, split_axis=0, concat_axis=0, tiled=True
        ).reshape(-1, LANES)

    sums = exchange(sums)
    packed, weights = pl.pallas_call(
        functools.partial(mix_kernel, slab_count=slab_count),
        in_specs=[whole()] * 4,
        out_specs=[whole(), whole()],
        out_shape=[
            jax.ShapeDtypeStruct((rows, LANES), f32),
            jax.ShapeDtypeStruct((8, LANES), f32),
        ],
        scratch_shapes=[
            pltpu.VMEM((z_local * y_local, x_length), bf16),
            pltpu.VMEM((z_local * y_local, x_length), bf16),
        ],
        compiler_params=params(24),
        name="mix",
    )(sums, held, *x_table)
    moved = exchange(packed)
    plane_in = pl.BlockSpec((histories, 1, y_local, x_length), lambda z: (0, z, 0, 0))
    mean, new_occupancy = pl.pallas_call(
        mean_kernel,
        grid=(z_local,),
        in_specs=[scalars(), scalars(), whole(), plane_in, whole(), whole()],
        out_specs=[pl.BlockSpec((1, y_local, x_length), lambda z: (z, 0, 0)), whole()],
        out_shape=[
            jax.ShapeDtypeStruct((z_local, y_local, x_length), f32),
            jax.ShapeDtypeStruct((slots, entries), f32),
        ],
        compiler_params=params(16),
        name="mean",
    )(species, slot_count, weights, density_history, occupancy_history, occupancy_residual)
    packed = pl.pallas_call(
        functools.partial(
            plane_kernel,
            slab_count=slab_count,
            pencil_count=pencil_count,
            z_local=z_local,
            y_local=y_local,
            x_length=x_length,
            scale=grid_mixing / cell_total,
        ),
        in_specs=[scalars()] + [whole()] * 5,
        out_specs=whole(),
        out_shape=jax.ShapeDtypeStruct((rows, LANES), f32),
        scratch_shapes=[
            pltpu.VMEM((y_length, z_length), f32),
            pltpu.VMEM((y_length, z_length // 2), f32),
        ],
        compiler_params=params(32),
        name="plane",
    )(place, moved, *z_table, *y_table)
    moved = exchange(packed)
    new_density = pl.pallas_call(
        functools.partial(x_inverse_kernel, slab_count=slab_count, pencil_count=pencil_count),
        in_specs=[whole()] * 4,
        out_specs=pl.BlockSpec(memory_space=pltpu.HBM),
        out_shape=jax.ShapeDtypeStruct((z_local * y_local, x_length), f32),
        scratch_shapes=[
            pltpu.VMEM((z_local * y_local, x_length), f32),
            pltpu.SemaphoreType.DMA((z_local * y_local // LANES,)),
        ],
        compiler_params=params(24),
        name="x_inverse",
    )(moved, mean.reshape(z_local * y_local, x_length), *x_table)
    return (new_density.reshape(z_local, y_local, x_length), new_occupancy)


def solution(mesh):
    torus = Mesh(
        mesh.devices.reshape(8, 4, 2, mesh.shape["pencil"]),
        ("slab_0", "slab_1", "slab_2", "pencil"),
    )
    placed = (
        P(None, SLAB, "pencil", None),
        P(None, SLAB, "pencil", None),
        P(None, SLAB_PENCIL, None),
        P(None, SLAB_PENCIL, None),
        P(SLAB_PENCIL),
        P(SLAB_PENCIL),
    )
    return jax.shard_map(
        body,
        mesh=torus,
        in_specs=placed,
        out_specs=(P(SLAB, "pencil", None), P(SLAB_PENCIL, None)),
        check_vma=False,
    )
```

```python
import functools
import math

import jax
import jax.numpy as jnp
import numpy as np
from jax import lax
from jax.experimental import pallas as pl
from jax.experimental.pallas import tpu as pltpu
from jax.sharding import Mesh
from jax.sharding import PartitionSpec as P

ORBITALS = 18
SLAB = ("slab_0", "slab_1", "slab_2")
SLAB_PENCIL = ("slab_0", "slab_1", "slab_2", "pencil")

grid_mixing = 0.5
block_mixing = 0.5
kerker_wave = 6.0
species_orbitals = (18, 13, 8, 5)

f32 = jnp.float32
bf16 = jnp.bfloat16
LANES = 128
MIB = 1 << 20


def pair_list(histories):
    return [(i, j) for i in range(histories) for j in range(i, histories)]


def split(value):
    high = value.astype(bf16)
    return high, (value - high.astype(f32)).astype(bf16)


def product(left, right, dims):
    dot = functools.partial(
        lax.dot_general, dimension_numbers=(dims, ((), ())), preferred_element_type=f32
    )
    return dot(left[0], right[0]) + (dot(left[0], right[1]) + dot(left[1], right[0]))


def hartley(rows, columns, length):
    angle = (np.outer(rows, columns) % length) * (2.0 * math.pi / length)
    table = np.cos(angle) + np.sin(angle)
    high = table.astype(bf16)
    low = (table - high.astype(np.float64)).astype(bf16)
    return high, low


def block_mask(species_ref, count_ref, slots, entries):
    row = lax.broadcasted_iota(jnp.int32, (slots, entries), 0)
    entry = lax.broadcasted_iota(jnp.int32, (slots, entries), 1)
    row_index = (entry * 3641) >> 16
    column_index = entry - ORBITALS * row_index
    limit = jnp.zeros((slots, entries), jnp.int32)
    for slot in range(slots):
        kind = species_ref[slot]
        number = jnp.int32(0)
        for index, orbital_number in enumerate(species_orbitals):
            number = jnp.where(kind == index, jnp.int32(orbital_number), number)
        number = jnp.where(slot < count_ref[0], number, jnp.int32(0))
        limit = jnp.where(row == slot, number, limit)
    return (row_index < limit) & (column_index < limit)


def parity_order(count):
    return np.concatenate([np.arange(0, count, 2), np.arange(1, count, 2)])


def parity_place(index, count):
    return index // 2 + (index % 2) * (count // 2)


def gram_kernel(
    species_ref,
    count_ref,
    residual_ref,
    block_ref,
    out_ref,
    held_ref,
    acc_ref,
    arrived,
    *,
    cell_total,
    block_total,
):
    histories, planes, rows, width = residual_ref.shape
    pairs = pair_list(histories)

    def fetch(z):
        return pltpu.make_async_copy(residual_ref.at[:, z], held_ref.at[:, z], arrived.at[z])

    for z in range(planes):
        fetch(z).start()
    acc_ref[...] = jnp.zeros_like(acc_ref)
    _, slots, entries = block_ref.shape
    mask = block_mask(species_ref, count_ref, slots, entries)
    blocks = [jnp.where(mask, block_ref[i], 0.0) for i in range(histories)]
    lane = lax.broadcasted_iota(jnp.int32, (1, LANES), 1)
    line = jnp.zeros((1, LANES), f32)
    for k, (i, j) in enumerate(pairs):
        block_part = jnp.sum(blocks[i] * blocks[j], axis=(0, 1), keepdims=True) / block_total
        line = jnp.where(lane == k, block_part, line)

    def plane(z, carry):
        fetch(z).wait()
        for start in range(0, width, LANES):
            lanes = slice(start, min(start + LANES, width))
            accs = [acc_ref[k, :, lanes] for k in range(len(pairs))]
            for top in range(0, rows, 8):
                values = [held_ref[i, z, top : top + 8, lanes] for i in range(histories)]
                accs = [acc + values[i] * values[j] for acc, (i, j) in zip(accs, pairs)]
            for k, acc in enumerate(accs):
                acc_ref[k, :, lanes] = acc
        return carry

    lax.fori_loop(0, planes, plane, 0)
    for k in range(len(pairs)):
        grid_part = jnp.sum(acc_ref[k], axis=(0, 1), keepdims=True) / cell_total
        line = jnp.where(lane == k, line + grid_part, line)
    out_ref[...] = jnp.broadcast_to(line, out_ref.shape)


def mixing_weights(line, histories):
    lane = lax.broadcasted_iota(jnp.int32, (1, LANES), 1)
    entry = {}
    for k, (i, j) in enumerate(pair_list(histories)):
        entry[j, i] = jnp.sum(jnp.where(lane == k, line, 0.0), axis=1, keepdims=True)
    factor = {}
    inverse = {}
    work = dict(entry)
    for k in range(histories):
        inverse[k] = 1.0 / work[k, k]
        for i in range(k + 1, histories):
            factor[i, k] = work[i, k] * inverse[k]
        for i in range(k + 1, histories):
            for j in range(k + 1, i + 1):
                work[i, j] = work[i, j] - factor[i, k] * work[j, k]
    solved = [jnp.ones((1, 1), f32) for _ in range(histories)]
    for i in range(histories):
        for k in range(i):
            solved[i] = solved[i] - factor[i, k] * solved[k]
    solved = [value * inverse[i] for i, value in enumerate(solved)]
    for i in reversed(range(histories)):
        for k in range(i + 1, histories):
            solved[i] = solved[i] - factor[k, i] * solved[k]
    total = solved[0]
    for value in solved[1:]:
        total = total + value
    return [value / total for value in solved]


def mix_kernel(
    sums_ref, residual_ref, high_ref, low_ref, out_ref, weights_ref, mixed_high, mixed_low, *, slab_count
):
    histories, planes, rows, _ = residual_ref.shape
    line = jnp.sum(sums_ref[...], axis=0, keepdims=True)
    weights = mixing_weights(line, histories)
    for i, weight in enumerate(weights):
        weights_ref[i : i + 1, :] = jnp.broadcast_to(weight, (1, LANES))
    weights_ref[histories:, :] = jnp.zeros((8 - histories, LANES), f32)
    for z in range(planes):
        mixed = weights[0] * residual_ref[0, z]
        for i in range(1, histories):
            mixed = mixed + weights[i] * residual_ref[i, z]
        high, low = split(mixed)
        here = pl.ds(parity_place(z, planes) * rows, rows)
        mixed_high[here, :] = high
        mixed_low[here, :] = low
    table = (high_ref[...], low_ref[...])
    result = product(table, (mixed_high[...], mixed_low[...]), ((1,), (1,)))
    pieces = result.shape[1] // LANES
    own_planes = result.shape[0] // slab_count - 1
    message = out_ref.shape[0] // (slab_count * own_planes)
    period = own_planes * message
    extra = message - pieces

    def put(row, plane, piece):
        out_ref[pl.ds(row, slab_count, stride=period), :] = result[
            plane * slab_count : (plane + 1) * slab_count, piece * LANES : (piece + 1) * LANES
        ]

    for own in range(own_planes):
        for piece in range(pieces):
            put(own * message + piece, own, piece)
        first = (pieces - extra) * (own // 2)
        for piece in range(extra):
            put(own * message + pieces + piece, own_planes, first + piece)


def plane_kernel(
    place_ref,
    in_ref,
    zh_ref,
    zl_ref,
    yh_ref,
    yl_ref,
    out_ref,
    main_ref,
    part_ref,
    *,
    slab_count,
    pencil_count,
    z_local,
    y_local,
    x_length,
    scale,
):
    z_length = slab_count * z_local
    y_length = pencil_count * y_local
    z_half = z_length // 2
    y_half = y_length // 2
    message = in_ref.shape[0] // (slab_count * pencil_count)
    period = pencil_count * message
    pieces = z_local * y_local // LANES
    extra = message - pieces
    half = z_local // 2
    half_rows = half * y_local
    spare = pieces * LANES - half_rows - (pieces - extra) * LANES
    in_half = place_ref[1] // 2
    out_half = place_ref[1] % 2

    def taken(row):
        return in_ref[pl.ds(row, slab_count, stride=period), :].T

    def spread(rows, count):
        return jnp.concatenate([rows[z * y_local : (z + 1) * y_local] for z in range(count)], axis=1)

    for q in range(pencil_count):
        here = slice(q * y_local, (q + 1) * y_local)
        rows = jnp.concatenate([taken(q * message + k) for k in range(pieces)], axis=0)
        main_ref[here, :] = spread(rows, z_local)
        rows = jnp.concatenate([taken(q * message + pieces + k) for k in range(extra)], axis=0)
        rows = jnp.where(in_half == 0, rows[:half_rows], rows[spare : spare + half_rows])
        part_ref[here, :] = spread(rows, half)

    def z_table(which):
        rows = pl.ds(pl.multiple_of(which * z_half, LANES), z_half)
        return (zh_ref[rows, :], zl_ref[rows, :])

    even = product(split(main_ref[:, :z_half]), z_table(0), ((1,), (0,)))
    odd = product(split(main_ref[:, z_half:]), z_table(1), ((1,), (0,)))
    part = product(split(part_ref[...]), z_table(in_half), ((1,), (0,)))
    lines = jnp.concatenate([even + odd, even - odd, part], axis=1)
    even = product((yh_ref[0], yl_ref[0]), split(lines[:y_half] + lines[y_half:]), ((1,), (0,)))
    odd = product((yh_ref[1], yl_ref[1]), split(lines[:y_half] - lines[y_half:]), ((1,), (0,)))
    spectrum = jnp.concatenate([even, odd], axis=0)

    row = lax.broadcasted_iota(jnp.int32, (y_length, z_length), 0)
    freq_y = jnp.where(row < y_half, 2 * row, 2 * row - (y_length - 1))
    freq_z = lax.broadcasted_iota(jnp.int32, (y_length, z_length), 1)
    mag_y = jnp.minimum(freq_y, y_length - freq_y).astype(f32)
    mag_z = jnp.minimum(freq_z, z_length - freq_z).astype(f32)
    plane = mag_y * mag_y + mag_z * mag_z

    def factor(own):
        freq_x = place_ref[0] * (pencil_count + 1) + own
        mag_x = jnp.minimum(freq_x, x_length - freq_x).astype(f32)
        square = plane + mag_x * mag_x
        return square / (square + kerker_wave * kerker_wave) * scale

    main = spectrum[:, :z_length] * factor(place_ref[1])
    shared = factor(pencil_count)
    same = jnp.where(in_half == out_half, 1.0, -1.0)
    part = spectrum[:, z_length:] * (shared[:, :z_half] + same * shared[:, z_half:])
    kept = jnp.concatenate(
        [main[:, :z_half] + main[:, z_half:], main[:, :z_half] - main[:, z_half:], part], axis=1
    )
    even = product((yh_ref[0], yl_ref[0]), split(kept[:y_half]), ((1,), (0,)))
    odd = product((yh_ref[2], yl_ref[2]), split(kept[y_half:]), ((1,), (0,)))
    lines = jnp.concatenate([even + odd, even - odd], axis=0)
    result = jnp.concatenate(
        [
            product(split(lines[:, :z_half]), z_table(0), ((1,), (1,))),
            product(split(lines[:, z_half:z_length]), z_table(1), ((1,), (1,))),
            product(split(lines[:, z_length:]), z_table(out_half), ((1,), (1,))),
        ],
        axis=1,
    )
    filler = jnp.zeros((extra * LANES - half_rows, slab_count), f32)
    for q in range(pencil_count):
        block = result[q * y_local : (q + 1) * y_local]
        rows = [
            block[:, z * slab_count : (z + 1) * slab_count] for z in range(z_local + half)
        ]
        rows = jnp.concatenate(rows + [filler], axis=0)
        for k in range(message):
            out_ref[pl.ds(q * message + k, slab_count, stride=period), :] = rows[
                k * LANES : (k + 1) * LANES
            ].T


def mean_kernel(
    species_ref, count_ref, weights_ref, density_ref, block_ref, block_residual_ref, out_ref, out_block_ref
):
    step = pl.program_id(0)
    histories = density_ref.shape[0]
    weights = [weights_ref[i : i + 1, 0:1] for i in range(histories)]
    mean = weights[0] * density_ref[0, 0]
    for i in range(1, histories):
        mean = mean + weights[i] * density_ref[i, 0]
    out_ref[0] = mean

    @pl.when(step == 0)
    def _():
        _, slots, entries = block_ref.shape
        mask = block_mask(species_ref, count_ref, slots, entries)
        total = weights[0] * (block_ref[0] + block_mixing * block_residual_ref[0])
        for i in range(1, histories):
            total = total + weights[i] * (block_ref[i] + block_mixing * block_residual_ref[i])
        out_block_ref[...] = jnp.where(mask, total, 0.0)


def x_inverse_kernel(
    in_ref,
    mean_ref,
    high_ref,
    low_ref,
    out_ref,
    field_ref,
    sent,
    *,
    slab_count,
    pencil_count,
    z_local,
):
    rows, x_length = mean_ref.shape
    y_local = rows // z_local
    table = (high_ref[...], low_ref[...])
    pieces = rows // LANES
    message = in_ref.shape[0] // (slab_count * pencil_count)
    order = [int(z) for z in parity_order(z_local)]

    def taken(row):
        return in_ref[pl.ds(row, slab_count, stride=pencil_count * message), :]

    halves = []
    for out_half in range(2):
        parts = [
            taken(out_half * message + k) + taken((out_half + 2) * message + k)
            for k in range(pieces, message)
        ]
        halves.append(jnp.concatenate(parts, axis=1)[:, : rows // 2])
    shared = jnp.concatenate(halves, axis=1)

    def send(place):
        source = field_ref.at[pl.ds(place * y_local, y_local)]
        target = out_ref.at[pl.ds(order[place] * y_local, y_local)]
        return pltpu.make_async_copy(source, target, sent.at[place])

    done = 0
    for piece in range(pieces):
        here = slice(piece * LANES, (piece + 1) * LANES)
        block = [taken(q * message + piece) for q in range(pencil_count)]
        block.append(shared[:, here])
        field = product(split(jnp.concatenate(block, axis=0).T), table, ((1,), (0,)))
        field_ref[here, :] = mean_ref[here, :] + field
        while (done + 1) * y_local <= (piece + 1) * LANES:
            send(done).start()
            done += 1
    for place in range(z_local):
        send(place).wait()


def whole():
    return pl.BlockSpec(memory_space=pltpu.VMEM)


def scalars():
    return pl.BlockSpec(memory_space=pltpu.SMEM)


def in_hbm(array):
    return pltpu.with_memory_space_constraint(array, pltpu.HBM)


def params(limit):
    return pltpu.CompilerParams(vmem_limit_bytes=limit * MIB)


def body(
    density_history, residual_history, occupancy_history, occupancy_residual, species, slot_count
):
    histories, z_local, y_local, x_length = residual_history.shape
    slab_count = lax.axis_size(SLAB)
    pencil_count = lax.axis_size("pencil")
    devices = slab_count * pencil_count
    y_length = y_local * pencil_count
    z_length = z_local * slab_count
    slots, entries = occupancy_residual.shape[1:]
    kx_local = x_length // slab_count
    message = z_local * y_local // LANES + -(-z_local * y_local // (2 * LANES))
    rows = devices * message
    cell_total = float(z_length * y_length * x_length)
    x_order = (np.arange(slab_count)[None, :] * kx_local + np.arange(kx_local)[:, None]).reshape(-1)
    x_table = hartley(x_order, np.arange(x_length), x_length)
    y_half = np.arange(y_length // 2)
    y_table = [
        np.stack(terms)
        for terms in zip(
            hartley(2 * y_half, y_half, y_length),
            hartley(2 * y_half + 1, y_half, y_length),
            hartley(y_half, 2 * y_half + 1, y_length),
        )
    ]
    z_order = (
        np.arange(slab_count)[None, :] * z_local + parity_order(z_local)[:, None]
    ).reshape(-1)
    z_table = hartley(z_order, np.arange(z_length // 2), z_length)
    place = jnp.stack([lax.axis_index(SLAB), lax.axis_index("pencil")]).astype(jnp.int32)
    place, species = lax.optimization_barrier((place, species))

    sums, held = pl.pallas_call(
        functools.partial(
            gram_kernel, cell_total=cell_total, block_total=100.0 * slots * devices
        ),
        in_specs=[scalars(), scalars(), pl.BlockSpec(memory_space=pltpu.HBM), whole()],
        out_specs=[whole(), whole()],
        out_shape=[
            jax.ShapeDtypeStruct((devices, LANES), f32),
            jax.ShapeDtypeStruct(residual_history.shape, f32),
        ],
        scratch_shapes=[
            pltpu.VMEM((len(pair_list(histories)), 8, x_length), f32),
            pltpu.SemaphoreType.DMA((z_local,)),
        ],
        compiler_params=params(16),
        name="gram",
    )(in_hbm(species), slot_count, in_hbm(residual_history), in_hbm(occupancy_residual))

    def exchange(array):
        return lax.all_to_all(
            array.reshape(devices, -1, 1, LANES), SLAB_PENCIL, split_axis=0, concat_axis=0, tiled=True
        ).reshape(-1, LANES)

    sums = exchange(sums)
    packed, weights = pl.pallas_call(
        functools.partial(mix_kernel, slab_count=slab_count),
        in_specs=[whole()] * 4,
        out_specs=[whole(), whole()],
        out_shape=[
            jax.ShapeDtypeStruct((rows, LANES), f32),
            jax.ShapeDtypeStruct((8, LANES), f32),
        ],
        scratch_shapes=[
            pltpu.VMEM((z_local * y_local, x_length), bf16),
            pltpu.VMEM((z_local * y_local, x_length), bf16),
        ],
        compiler_params=params(24),
        name="mix",
    )(sums, held, *x_table)
    moved = exchange(packed)
    plane_in = pl.BlockSpec((histories, 1, y_local, x_length), lambda z: (0, z, 0, 0))
    mean, new_occupancy = pl.pallas_call(
        mean_kernel,
        grid=(z_local,),
        in_specs=[scalars(), scalars(), whole(), plane_in, whole(), whole()],
        out_specs=[
            pl.BlockSpec((1, y_local, x_length), lambda z: (parity_place(z, z_local), 0, 0)),
            whole(),
        ],
        out_shape=[
            jax.ShapeDtypeStruct((z_local, y_local, x_length), f32),
            jax.ShapeDtypeStruct((slots, entries), f32),
        ],
        compiler_params=params(16),
        name="mean",
    )(species, slot_count, weights, density_history, occupancy_history, occupancy_residual)
    packed = pl.pallas_call(
        functools.partial(
            plane_kernel,
            slab_count=slab_count,
            pencil_count=pencil_count,
            z_local=z_local,
            y_local=y_local,
            x_length=x_length,
            scale=grid_mixing / cell_total,
        ),
        in_specs=[scalars()] + [whole()] * 5,
        out_specs=whole(),
        out_shape=jax.ShapeDtypeStruct((rows, LANES), f32),
        scratch_shapes=[
            pltpu.VMEM((y_length, z_length), f32),
            pltpu.VMEM((y_length, z_length // 2), f32),
        ],
        compiler_params=params(32),
        name="plane",
    )(place, moved, *z_table, *y_table)
    moved = exchange(packed)
    new_density = pl.pallas_call(
        functools.partial(
            x_inverse_kernel, slab_count=slab_count, pencil_count=pencil_count, z_local=z_local
        ),
        in_specs=[whole()] * 4,
        out_specs=pl.BlockSpec(memory_space=pltpu.HBM),
        out_shape=jax.ShapeDtypeStruct((z_local * y_local, x_length), f32),
        scratch_shapes=[
            pltpu.VMEM((z_local * y_local, x_length), f32),
            pltpu.SemaphoreType.DMA((z_local,)),
        ],
        compiler_params=params(24),
        name="x_inverse",
    )(moved, mean.reshape(z_local * y_local, x_length), *x_table)
    return (new_density.reshape(z_local, y_local, x_length), new_occupancy)


def solution(mesh):
    torus = Mesh(
        mesh.devices.reshape(8, 4, 2, mesh.shape["pencil"]),
        ("slab_0", "slab_1", "slab_2", "pencil"),
    )
    placed = (
        P(None, SLAB, "pencil", None),
        P(None, SLAB, "pencil", None),
        P(None, SLAB_PENCIL, None),
        P(None, SLAB_PENCIL, None),
        P(SLAB_PENCIL),
        P(SLAB_PENCIL),
    )
    return jax.shard_map(
        body,
        mesh=torus,
        in_specs=placed,
        out_specs=(P(SLAB, "pencil", None), P(SLAB_PENCIL, None)),
        check_vma=False,
    )
```

```python
import functools
import math

import jax
import jax.numpy as jnp
import numpy as np
from jax import lax
from jax.experimental import pallas as pl
from jax.experimental.pallas import tpu as pltpu
from jax.sharding import Mesh
from jax.sharding import PartitionSpec as P

ORBITALS = 18
SLAB = ("slab_0", "slab_1", "slab_2")
SLAB_PENCIL = ("slab_0", "slab_1", "slab_2", "pencil")

grid_mixing = 0.5
block_mixing = 0.5
kerker_wave = 6.0
species_orbitals = (18, 13, 8, 5)

f32 = jnp.float32
bf16 = jnp.bfloat16
LANES = 128
MIB = 1 << 20
FETCH_AHEAD = 4


def pair_list(histories):
    return [(i, j) for i in range(histories) for j in range(i, histories)]


def split(value):
    high = value.astype(bf16)
    return high, (value - high.astype(f32)).astype(bf16)


def product(left, right, dims):
    dot = functools.partial(
        lax.dot_general, dimension_numbers=(dims, ((), ())), preferred_element_type=f32
    )
    return dot(left[0], right[0]) + (dot(left[0], right[1]) + dot(left[1], right[0]))


def hartley(rows, columns, length):
    angle = (np.outer(rows, columns) % length) * (2.0 * math.pi / length)
    table = np.cos(angle) + np.sin(angle)
    high = table.astype(bf16)
    low = (table - high.astype(np.float64)).astype(bf16)
    return high, low


def block_mask(species_ref, count_ref, slots, entries):
    row = lax.broadcasted_iota(jnp.int32, (slots, entries), 0)
    entry = lax.broadcasted_iota(jnp.int32, (slots, entries), 1)
    row_index = (entry * 3641) >> 16
    column_index = entry - ORBITALS * row_index
    limit = jnp.zeros((slots, entries), jnp.int32)
    for slot in range(slots):
        kind = species_ref[slot]
        number = jnp.int32(0)
        for index, orbital_number in enumerate(species_orbitals):
            number = jnp.where(kind == index, jnp.int32(orbital_number), number)
        number = jnp.where(slot < count_ref[0], number, jnp.int32(0))
        limit = jnp.where(row == slot, number, limit)
    return (row_index < limit) & (column_index < limit)


def gram_kernel(
    species_ref,
    count_ref,
    residual_ref,
    block_ref,
    out_ref,
    held_ref,
    acc_ref,
    arrived,
    *,
    cell_total,
    block_total,
):
    histories, planes, rows, width = residual_ref.shape
    pairs = pair_list(histories)

    def fetch(z):
        return pltpu.make_async_copy(residual_ref.at[:, z], held_ref.at[:, z], arrived.at[z])

    ahead = min(FETCH_AHEAD, planes)
    for z in range(ahead):
        fetch(z).start()
    acc_ref[...] = jnp.zeros_like(acc_ref)
    _, slots, entries = block_ref.shape
    mask = block_mask(species_ref, count_ref, slots, entries)
    blocks = [jnp.where(mask, block_ref[i], 0.0) for i in range(histories)]
    lane = lax.broadcasted_iota(jnp.int32, (1, LANES), 1)
    line = jnp.zeros((1, LANES), f32)
    for k, (i, j) in enumerate(pairs):
        block_part = jnp.sum(blocks[i] * blocks[j], axis=(0, 1), keepdims=True) / block_total
        line = jnp.where(lane == k, block_part, line)

    def plane(z, carry):
        @pl.when(z + ahead < planes)
        def _():
            fetch(z + ahead).start()

        fetch(z).wait()
        for start in range(0, width, LANES):
            lanes = slice(start, min(start + LANES, width))
            accs = [acc_ref[k, :, lanes] for k in range(len(pairs))]
            for top in range(0, rows, 8):
                values = [held_ref[i, z, top : top + 8, lanes] for i in range(histories)]
                accs = [acc + values[i] * values[j] for acc, (i, j) in zip(accs, pairs)]
            for k, acc in enumerate(accs):
                acc_ref[k, :, lanes] = acc
        return carry

    lax.fori_loop(0, planes, plane, 0)
    for k in range(len(pairs)):
        grid_part = jnp.sum(acc_ref[k], axis=(0, 1), keepdims=True) / cell_total
        line = jnp.where(lane == k, line + grid_part, line)
    out_ref[...] = jnp.broadcast_to(line, out_ref.shape)


def mixing_weights(line, histories):
    lane = lax.broadcasted_iota(jnp.int32, (1, LANES), 1)
    entry = {}
    for k, (i, j) in enumerate(pair_list(histories)):
        entry[j, i] = jnp.sum(jnp.where(lane == k, line, 0.0), axis=1, keepdims=True)
    factor = {}
    inverse = {}
    work = dict(entry)
    for k in range(histories):
        inverse[k] = 1.0 / work[k, k]
        for i in range(k + 1, histories):
            factor[i, k] = work[i, k] * inverse[k]
        for i in range(k + 1, histories):
            for j in range(k + 1, i + 1):
                work[i, j] = work[i, j] - factor[i, k] * work[j, k]
    solved = [jnp.ones((1, 1), f32) for _ in range(histories)]
    for i in range(histories):
        for k in range(i):
            solved[i] = solved[i] - factor[i, k] * solved[k]
    solved = [value * inverse[i] for i, value in enumerate(solved)]
    for i in reversed(range(histories)):
        for k in range(i + 1, histories):
            solved[i] = solved[i] - factor[k, i] * solved[k]
    total = solved[0]
    for value in solved[1:]:
        total = total + value
    return [value / total for value in solved]


def mix_kernel(
    sums_ref, residual_ref, high_ref, low_ref, out_ref, weights_ref, mixed_high, mixed_low, *, slab_count
):
    histories, planes, rows, _ = residual_ref.shape
    line = jnp.sum(sums_ref[...], axis=0, keepdims=True)
    weights = mixing_weights(line, histories)
    for i, weight in enumerate(weights):
        weights_ref[i : i + 1, :] = jnp.broadcast_to(weight, (1, LANES))
    weights_ref[histories:, :] = jnp.zeros((8 - histories, LANES), f32)
    for z in range(planes):
        mixed = weights[0] * residual_ref[0, z]
        for i in range(1, histories):
            mixed = mixed + weights[i] * residual_ref[i, z]
        high, low = split(mixed)
        filler = jnp.zeros((LANES - rows, mixed.shape[1]), bf16)
        mixed_high[z * LANES : z * LANES + rows, :] = high
        mixed_high[z * LANES + rows : (z + 1) * LANES, :] = filler
        mixed_low[z * LANES : z * LANES + rows, :] = low
        mixed_low[z * LANES + rows : (z + 1) * LANES, :] = filler
    table = (high_ref[...], low_ref[...])
    result = product(table, (mixed_high[...], mixed_low[...]), ((1,), (1,)))
    own_planes = result.shape[0] // slab_count - 1
    period = own_planes * planes
    part = rows // 2
    lane = lax.broadcasted_iota(jnp.int32, (slab_count, LANES), 1)
    here = (lane >= rows) & (lane < rows + part)
    for z in range(planes):
        columns = slice(z * LANES, (z + 1) * LANES)
        shared = result[own_planes * slab_count :, columns]
        shared = [
            jnp.where(here, pltpu.roll(shared, shift, 1), 0.0) for shift in (rows, rows - part)
        ]
        for own in range(own_planes):
            out_ref[pl.ds(own * planes + z, slab_count, stride=period), :] = (
                result[own * slab_count : (own + 1) * slab_count, columns] + shared[own // 2]
            )


def plane_kernel(
    place_ref,
    in_ref,
    zh_ref,
    zl_ref,
    yh_ref,
    yl_ref,
    out_ref,
    *,
    x_length,
    y_length,
    z_length,
    scale,
):
    slab_count, pencil_count, z_local, _ = in_ref.shape
    z_half = z_length // 2
    y_half = y_length // 2
    s_half = slab_count // 2
    fold = pencil_count // 2 * LANES
    in_half = place_ref[1] // 2
    out_half = place_ref[1] % 2

    def gathered(first):
        return jnp.concatenate(
            [
                in_ref[first : first + s_half, q].reshape(z_half, LANES)
                for q in range(pencil_count)
            ],
            axis=1,
        )

    def z_table(kind):
        return (zh_ref[kind], zl_ref[kind])

    def y_table(half, kind):
        return (yh_ref[2 * half + kind], yl_ref[2 * half + kind])

    low, high = gathered(0), gathered(s_half)
    lines = jnp.concatenate(
        [
            product(z_table(0), split(low + high), ((1,), (0,))),
            product(z_table(1), split(low - high), ((1,), (0,))),
        ],
        axis=0,
    )
    folded = [lines[:, :fold] + lines[:, fold:], lines[:, :fold] - lines[:, fold:]]
    row = lax.broadcasted_iota(jnp.int32, (z_length, 1), 0)
    lane = lax.broadcasted_iota(jnp.int32, (1, y_length), 1)
    freq_z = jnp.where(row < z_half, 2 * row, 2 * row - (z_length - 1))
    first_x = place_ref[0] * (pencil_count + 1)
    freq_x = jnp.where(lane < y_half, first_x + place_ref[1], first_x + pencil_count)

    def squared(index, length):
        least = jnp.minimum(index, length - index).astype(f32)
        return least * least

    results = []
    for kind in range(2):
        spectrum = product(split(folded[kind]), y_table(in_half, kind), ((1,), (0,)))
        freq_y = 2 * jnp.where(lane < y_half, lane, lane - y_half) + kind
        square = squared(freq_z, z_length) + (
            squared(freq_y, y_length) + squared(freq_x, x_length)
        )
        kept = spectrum * (square / (square + kerker_wave * kerker_wave) * scale)
        results.append(product(split(kept), y_table(out_half, kind), ((1,), (1,))))
    lines = jnp.concatenate([results[0] + results[1], results[0] - results[1]], axis=1)
    even = product(z_table(0), split(lines[:z_half]), ((1,), (0,)))
    odd = product(z_table(1), split(lines[z_half:]), ((0,), (0,)))
    low, high = even + odd, even - odd
    for q in range(pencil_count):
        columns = slice(q * LANES, (q + 1) * LANES)
        out_ref[:s_half, q] = low[:, columns].reshape(s_half, z_local, LANES)
        out_ref[s_half:, q] = high[:, columns].reshape(s_half, z_local, LANES)


def mean_kernel(
    species_ref, count_ref, weights_ref, density_ref, block_ref, block_residual_ref, out_ref, out_block_ref
):
    step = pl.program_id(0)
    histories = density_ref.shape[0]
    weights = [weights_ref[i : i + 1, 0:1] for i in range(histories)]
    mean = weights[0] * density_ref[0, 0]
    for i in range(1, histories):
        mean = mean + weights[i] * density_ref[i, 0]
    out_ref[0] = mean

    @pl.when(step == 0)
    def _():
        _, slots, entries = block_ref.shape
        mask = block_mask(species_ref, count_ref, slots, entries)
        total = weights[0] * (block_ref[0] + block_mixing * block_residual_ref[0])
        for i in range(1, histories):
            total = total + weights[i] * (block_ref[i] + block_mixing * block_residual_ref[i])
        out_block_ref[...] = jnp.where(mask, total, 0.0)


def x_inverse_kernel(
    in_ref,
    mean_ref,
    high_ref,
    low_ref,
    out_ref,
    field_ref,
    sent,
    *,
    slab_count,
    pencil_count,
    z_local,
):
    rows, x_length = mean_ref.shape
    y_local = rows // z_local
    part = y_local // 2
    table = (high_ref[...], low_ref[...])
    lane = lax.broadcasted_iota(jnp.int32, (slab_count, LANES), 1)
    groups = sent.shape[0]
    group = z_local // groups

    def send(index):
        here = pl.ds(index * group * y_local, group * y_local)
        return pltpu.make_async_copy(field_ref.at[here], out_ref.at[here], sent.at[index])

    for index in range(groups):
        lines = []
        for z in range(index * group, (index + 1) * group):
            block = [
                in_ref[pl.ds(q * z_local + z, slab_count, stride=pencil_count * z_local), :]
                for q in range(pencil_count)
            ]
            first = pltpu.roll(block[0] + block[2], LANES - y_local, 1)
            second = pltpu.roll(block[1] + block[3], LANES - y_local + part, 1)
            block.append(jnp.where(lane < part, first, second))
            lines.append(jnp.concatenate(block, axis=0).T[:y_local])
        lines = jnp.concatenate(lines, axis=0)
        field = product(split(lines), table, ((1,), (0,)))
        here = slice(index * group * y_local, (index + 1) * group * y_local)
        field_ref[here, :] = mean_ref[here, :] + field
        send(index).start()
    for index in range(groups):
        send(index).wait()


def whole():
    return pl.BlockSpec(memory_space=pltpu.VMEM)


def scalars():
    return pl.BlockSpec(memory_space=pltpu.SMEM)


def in_hbm(array):
    return pltpu.with_memory_space_constraint(array, pltpu.HBM)


def params(limit):
    return pltpu.CompilerParams(vmem_limit_bytes=limit * MIB)


def body(
    density_history, residual_history, occupancy_history, occupancy_residual, species, slot_count
):
    histories, z_local, y_local, x_length = residual_history.shape
    slab_count = lax.axis_size(SLAB)
    pencil_count = lax.axis_size("pencil")
    devices = slab_count * pencil_count
    y_length = y_local * pencil_count
    z_length = z_local * slab_count
    slots, entries = occupancy_residual.shape[1:]
    kx_local = x_length // slab_count
    rows = devices * z_local
    part = y_local // 2
    cell_total = float(z_length * y_length * x_length)
    x_order = (np.arange(slab_count)[None, :] * kx_local + np.arange(kx_local)[:, None]).reshape(-1)
    x_table = hartley(x_order, np.arange(x_length), x_length)
    y_tables = []
    for half in range(2):
        for kind in range(2):
            freq = 2 * np.arange(y_length // 2) + kind
            terms = [np.zeros((pencil_count // 2, LANES, 2, y_length // 2), bf16) for _ in range(2)]
            for q in range(pencil_count // 2):
                point = q * y_local + np.arange(y_local)
                whole_terms = hartley(point, freq, y_length)
                part_terms = hartley(point[half * part : (half + 1) * part], freq, y_length)
                for term, own, some in zip(terms, whole_terms, part_terms):
                    term[q, :y_local, 0] = own
                    term[q, y_local : y_local + part, 1] = some
            y_tables.append([term.reshape(-1, y_length) for term in terms])
    y_table = [np.stack(terms) for terms in zip(*y_tables)]
    z_half = np.arange(z_length // 2)
    z_table = [
        np.stack(terms)
        for terms in zip(
            hartley(2 * z_half, z_half, z_length),
            hartley(2 * z_half + 1, z_half, z_length),
        )
    ]
    place = jnp.stack([lax.axis_index(SLAB), lax.axis_index("pencil")]).astype(jnp.int32)
    place, species = lax.optimization_barrier((place, species))

    sums, held = pl.pallas_call(
        functools.partial(
            gram_kernel, cell_total=cell_total, block_total=100.0 * slots * devices
        ),
        in_specs=[scalars(), scalars(), pl.BlockSpec(memory_space=pltpu.HBM), whole()],
        out_specs=[whole(), whole()],
        out_shape=[
            jax.ShapeDtypeStruct((devices, LANES), f32),
            jax.ShapeDtypeStruct(residual_history.shape, f32),
        ],
        scratch_shapes=[
            pltpu.VMEM((len(pair_list(histories)), 8, x_length), f32),
            pltpu.SemaphoreType.DMA((z_local,)),
        ],
        compiler_params=params(16),
        name="gram",
    )(in_hbm(species), slot_count, in_hbm(residual_history), in_hbm(occupancy_residual))

    def exchange(array):
        return lax.all_to_all(
            array.reshape(devices, -1, LANES), SLAB_PENCIL, split_axis=0, concat_axis=0, tiled=True
        )

    sums = exchange(sums).reshape(devices, LANES)
    packed, weights = pl.pallas_call(
        functools.partial(mix_kernel, slab_count=slab_count),
        in_specs=[whole()] * 4,
        out_specs=[whole(), whole()],
        out_shape=[
            jax.ShapeDtypeStruct((rows, LANES), f32),
            jax.ShapeDtypeStruct((8, LANES), f32),
        ],
        scratch_shapes=[
            pltpu.VMEM((z_local * LANES, x_length), bf16),
            pltpu.VMEM((z_local * LANES, x_length), bf16),
        ],
        compiler_params=params(24),
        name="mix",
    )(sums, held, *x_table)
    moved = exchange(packed).reshape(slab_count, pencil_count, z_local, LANES)
    plane_in = pl.BlockSpec((histories, 1, y_local, x_length), lambda z: (0, z, 0, 0))
    mean, new_occupancy = pl.pallas_call(
        mean_kernel,
        grid=(z_local,),
        in_specs=[scalars(), scalars(), whole(), plane_in, whole(), whole()],
        out_specs=[
            pl.BlockSpec((1, y_local, x_length), lambda z: (z, 0, 0)),
            whole(),
        ],
        out_shape=[
            jax.ShapeDtypeStruct((z_local, y_local, x_length), f32),
            jax.ShapeDtypeStruct((slots, entries), f32),
        ],
        compiler_params=params(16),
        name="mean",
    )(species, slot_count, weights, density_history, occupancy_history, occupancy_residual)
    packed = pl.pallas_call(
        functools.partial(
            plane_kernel,
            x_length=x_length,
            y_length=y_length,
            z_length=z_length,
            scale=grid_mixing / cell_total,
        ),
        in_specs=[scalars()] + [whole()] * 5,
        out_specs=whole(),
        out_shape=jax.ShapeDtypeStruct((slab_count, pencil_count, z_local, LANES), f32),
        compiler_params=params(32),
        name="plane",
    )(place, moved, *z_table, *y_table)
    moved = exchange(packed).reshape(rows, LANES)
    new_density = pl.pallas_call(
        functools.partial(
            x_inverse_kernel, slab_count=slab_count, pencil_count=pencil_count, z_local=z_local
        ),
        in_specs=[whole()] * 4,
        out_specs=pl.BlockSpec(memory_space=pltpu.HBM),
        out_shape=jax.ShapeDtypeStruct((z_local * y_local, x_length), f32),
        scratch_shapes=[
            pltpu.VMEM((z_local * y_local, x_length), f32),
            pltpu.SemaphoreType.DMA((2,)),
        ],
        compiler_params=params(24),
        name="x_inverse",
    )(moved, mean.reshape(z_local * y_local, x_length), *x_table)
    return (new_density.reshape(z_local, y_local, x_length), new_occupancy)


def solution(mesh):
    torus = Mesh(
        mesh.devices.reshape(8, 4, 2, mesh.shape["pencil"]),
        ("slab_0", "slab_1", "slab_2", "pencil"),
    )
    placed = (
        P(None, SLAB, "pencil", None),
        P(None, SLAB, "pencil", None),
        P(None, SLAB_PENCIL, None),
        P(None, SLAB_PENCIL, None),
        P(SLAB_PENCIL),
        P(SLAB_PENCIL),
    )
    return jax.shard_map(
        body,
        mesh=torus,
        in_specs=placed,
        out_specs=(P(SLAB, "pencil", None), P(SLAB_PENCIL, None)),
        check_vma=False,
    )
```

```python
import functools
import math

import jax
import jax.numpy as jnp
import numpy as np
from jax import lax
from jax.experimental import pallas as pl
from jax.experimental.pallas import tpu as pltpu
from jax.sharding import Mesh
from jax.sharding import PartitionSpec as P

ORBITALS = 18
SLAB = ("slab_0", "slab_1", "slab_2")
SLAB_PENCIL = ("slab_0", "slab_1", "slab_2", "pencil")

grid_mixing = 0.5
block_mixing = 0.5
kerker_wave = 6.0
species_orbitals = (18, 13, 8, 5)

f32 = jnp.float32
bf16 = jnp.bfloat16
LANES = 128
MIB = 1 << 20


def pair_list(histories):
    return [(i, j) for i in range(histories) for j in range(i, histories)]


def split(value):
    high = value.astype(bf16)
    return high, (value - high.astype(f32)).astype(bf16)


def product(left, right, dims):
    dot = functools.partial(
        lax.dot_general, dimension_numbers=(dims, ((), ())), preferred_element_type=f32
    )
    return dot(left[0], right[0]) + (dot(left[0], right[1]) + dot(left[1], right[0]))


def hartley(rows, columns, length):
    angle = (np.outer(rows, columns) % length) * (2.0 * math.pi / length)
    table = np.cos(angle) + np.sin(angle)
    high = table.astype(bf16)
    low = (table - high.astype(np.float64)).astype(bf16)
    return high, low


def block_mask(species_ref, count_ref, slots, entries):
    row = lax.broadcasted_iota(jnp.int32, (slots, entries), 0)
    entry = lax.broadcasted_iota(jnp.int32, (slots, entries), 1)
    row_index = (entry * 3641) >> 16
    column_index = entry - ORBITALS * row_index
    limit = jnp.zeros((slots, entries), jnp.int32)
    for slot in range(slots):
        kind = species_ref[slot]
        number = jnp.int32(0)
        for index, orbital_number in enumerate(species_orbitals):
            number = jnp.where(kind == index, jnp.int32(orbital_number), number)
        number = jnp.where(slot < count_ref[0], number, jnp.int32(0))
        limit = jnp.where(row == slot, number, limit)
    return (row_index < limit) & (column_index < limit)


def gram_kernel(
    species_ref,
    count_ref,
    residual_ref,
    block_ref,
    out_ref,
    held_ref,
    acc_ref,
    arrived,
    *,
    cell_total,
    block_total,
):
    histories, planes, rows, width = residual_ref.shape
    pairs = pair_list(histories)

    def fetch(z):
        return pltpu.make_async_copy(residual_ref.at[:, z], held_ref.at[:, z], arrived.at[z])

    for z in range(planes):
        fetch(z).start()
    acc_ref[...] = jnp.zeros_like(acc_ref)
    _, slots, entries = block_ref.shape
    mask = block_mask(species_ref, count_ref, slots, entries)
    blocks = [jnp.where(mask, block_ref[i], 0.0) for i in range(histories)]
    lane = lax.broadcasted_iota(jnp.int32, (1, LANES), 1)
    line = jnp.zeros((1, LANES), f32)
    for k, (i, j) in enumerate(pairs):
        block_part = jnp.sum(blocks[i] * blocks[j], axis=(0, 1), keepdims=True) / block_total
        line = jnp.where(lane == k, block_part, line)

    def plane(z, carry):
        fetch(z).wait()
        for start in range(0, width, LANES):
            lanes = slice(start, min(start + LANES, width))
            accs = [acc_ref[k, :, lanes] for k in range(len(pairs))]
            for top in range(0, rows, 8):
                values = [held_ref[i, z, top : top + 8, lanes] for i in range(histories)]
                accs = [acc + values[i] * values[j] for acc, (i, j) in zip(accs, pairs)]
            for k, acc in enumerate(accs):
                acc_ref[k, :, lanes] = acc
        return carry

    lax.fori_loop(0, planes, plane, 0)
    for k in range(len(pairs)):
        grid_part = jnp.sum(acc_ref[k], axis=(0, 1), keepdims=True) / cell_total
        line = jnp.where(lane == k, line + grid_part, line)
    out_ref[...] = jnp.broadcast_to(line, out_ref.shape)


def mixing_weights(line, histories):
    lane = lax.broadcasted_iota(jnp.int32, (1, LANES), 1)
    entry = {}
    for k, (i, j) in enumerate(pair_list(histories)):
        entry[j, i] = jnp.sum(jnp.where(lane == k, line, 0.0), axis=1, keepdims=True)
    factor = {}
    inverse = {}
    work = dict(entry)
    for k in range(histories):
        inverse[k] = 1.0 / work[k, k]
        for i in range(k + 1, histories):
            factor[i, k] = work[i, k] * inverse[k]
        for i in range(k + 1, histories):
            for j in range(k + 1, i + 1):
                work[i, j] = work[i, j] - factor[i, k] * work[j, k]
    solved = [jnp.ones((1, 1), f32) for _ in range(histories)]
    for i in range(histories):
        for k in range(i):
            solved[i] = solved[i] - factor[i, k] * solved[k]
    solved = [value * inverse[i] for i, value in enumerate(solved)]
    for i in reversed(range(histories)):
        for k in range(i + 1, histories):
            solved[i] = solved[i] - factor[k, i] * solved[k]
    total = solved[0]
    for value in solved[1:]:
        total = total + value
    return [value / total for value in solved]


def mix_kernel(
    sums_ref, residual_ref, high_ref, low_ref, out_ref, weights_ref, mixed_high, mixed_low, *, slab_count
):
    histories, planes, rows, _ = residual_ref.shape
    line = jnp.sum(sums_ref[...], axis=0, keepdims=True)
    weights = mixing_weights(line, histories)
    for i, weight in enumerate(weights):
        weights_ref[i : i + 1, :] = jnp.broadcast_to(weight, (1, LANES))
    weights_ref[histories:, :] = jnp.zeros((8 - histories, LANES), f32)
    for z in range(planes):
        mixed = weights[0] * residual_ref[0, z]
        for i in range(1, histories):
            mixed = mixed + weights[i] * residual_ref[i, z]
        high, low = split(mixed)
        filler = jnp.zeros((LANES - rows, mixed.shape[1]), bf16)
        mixed_high[z * LANES : z * LANES + rows, :] = high
        mixed_high[z * LANES + rows : (z + 1) * LANES, :] = filler
        mixed_low[z * LANES : z * LANES + rows, :] = low
        mixed_low[z * LANES + rows : (z + 1) * LANES, :] = filler
    table = (high_ref[...], low_ref[...])
    result = product(table, (mixed_high[...], mixed_low[...]), ((1,), (1,)))
    own_planes = result.shape[0] // slab_count - 1
    part = rows // 2
    lane = lax.broadcasted_iota(jnp.int32, (slab_count, LANES), 1)
    here = (lane >= rows) & (lane < rows + part)
    shared = []
    for shift in (rows, rows - part):
        shared.append(
            [
                jnp.where(
                    here,
                    pltpu.roll(
                        result[own_planes * slab_count :, z * LANES : (z + 1) * LANES], shift, 1
                    ),
                    0.0,
                )
                for z in range(planes)
            ]
        )
    for own in range(own_planes):
        lines = [
            result[own * slab_count : (own + 1) * slab_count, z * LANES : (z + 1) * LANES]
            + shared[own // 2][z]
            for z in range(planes)
        ]
        out_ref[:, own] = jnp.swapaxes(jnp.stack(lines), 0, 1)


def plane_kernel(
    place_ref,
    in_ref,
    zh_ref,
    zl_ref,
    yh_ref,
    yl_ref,
    out_ref,
    made_ref,
    sent,
    *,
    x_length,
    y_length,
    z_length,
    scale,
):
    slab_count, pencil_count, z_local, _ = in_ref.shape
    z_half = z_length // 2
    y_half = y_length // 2
    s_half = slab_count // 2
    fold = pencil_count // 2 * LANES
    in_half = place_ref[1] // 2
    out_half = place_ref[1] % 2

    def gathered(first):
        return jnp.concatenate(
            [
                in_ref[first : first + s_half, q].reshape(z_half, LANES)
                for q in range(pencil_count)
            ],
            axis=1,
        )

    def z_table(kind):
        return (zh_ref[kind], zl_ref[kind])

    def y_table(half, kind):
        return (yh_ref[2 * half + kind], yl_ref[2 * half + kind])

    low, high = gathered(0), gathered(s_half)
    lines = jnp.concatenate(
        [
            product(z_table(0), split(low + high), ((1,), (0,))),
            product(z_table(1), split(low - high), ((1,), (0,))),
        ],
        axis=0,
    )
    folded = [lines[:, :fold] + lines[:, fold:], lines[:, :fold] - lines[:, fold:]]
    row = lax.broadcasted_iota(jnp.int32, (z_length, 1), 0)
    lane = lax.broadcasted_iota(jnp.int32, (1, y_length), 1)
    freq_z = jnp.where(row < z_half, 2 * row, 2 * row - (z_length - 1))
    first_x = place_ref[0] * (pencil_count + 1)
    freq_x = jnp.where(lane < y_half, first_x + place_ref[1], first_x + pencil_count)

    def squared(index, length):
        least = jnp.minimum(index, length - index).astype(f32)
        return least * least

    results = []
    for kind in range(2):
        spectrum = product(split(folded[kind]), y_table(in_half, kind), ((1,), (0,)))
        freq_y = 2 * jnp.where(lane < y_half, lane, lane - y_half) + kind
        square = squared(freq_z, z_length) + (
            squared(freq_y, y_length) + squared(freq_x, x_length)
        )
        kept = spectrum * (square / (square + kerker_wave * kerker_wave) * scale)
        results.append(product(split(kept), y_table(out_half, kind), ((1,), (1,))))
    lines = jnp.concatenate([results[0] + results[1], results[0] - results[1]], axis=1)
    sends = []
    for q in range(pencil_count):
        for first in (0, s_half):
            here = pl.ds(first, s_half)
            sends.append(
                pltpu.make_async_copy(
                    made_ref.at[here, q], out_ref.at[here, q], sent.at[len(sends)]
                )
            )
    for start in range(0, pencil_count, 2):
        columns = slice(start * LANES, (start + 2) * LANES)
        even = product(z_table(0), split(lines[:z_half, columns]), ((1,), (0,)))
        odd = product(z_table(1), split(lines[z_half:, columns]), ((0,), (0,)))
        low, high = even + odd, even - odd
        for q in (start, start + 1):
            columns = slice((q - start) * LANES, (q - start + 1) * LANES)
            made_ref[:s_half, q] = low[:, columns].reshape(s_half, z_local, LANES)
            sends[2 * q].start()
            made_ref[s_half:, q] = high[:, columns].reshape(s_half, z_local, LANES)
            sends[2 * q + 1].start()
    for send in sends:
        send.wait()


def mean_kernel(
    species_ref, count_ref, weights_ref, density_ref, block_ref, block_residual_ref, out_ref, out_block_ref
):
    step = pl.program_id(0)
    histories = density_ref.shape[0]
    weights = [weights_ref[i : i + 1, 0:1] for i in range(histories)]
    mean = weights[0] * density_ref[0, 0]
    for i in range(1, histories):
        mean = mean + weights[i] * density_ref[i, 0]
    out_ref[0] = mean

    @pl.when(step == 0)
    def _():
        _, slots, entries = block_ref.shape
        mask = block_mask(species_ref, count_ref, slots, entries)
        total = weights[0] * (block_ref[0] + block_mixing * block_residual_ref[0])
        for i in range(1, histories):
            total = total + weights[i] * (block_ref[i] + block_mixing * block_residual_ref[i])
        out_block_ref[...] = jnp.where(mask, total, 0.0)


def x_inverse_kernel(
    in_ref,
    mean_ref,
    high_ref,
    low_ref,
    out_ref,
    field_ref,
    sent,
    *,
    slab_count,
    pencil_count,
    z_local,
):
    rows, x_length = mean_ref.shape
    y_local = rows // z_local
    part = y_local // 2
    table = (high_ref[...], low_ref[...])
    lane = lax.broadcasted_iota(jnp.int32, (slab_count, LANES), 1)
    groups = sent.shape[0]
    group = z_local // groups

    def send(index):
        here = pl.ds(index * group * y_local, group * y_local)
        return pltpu.make_async_copy(field_ref.at[here], out_ref.at[here], sent.at[index])

    blocks = [jnp.swapaxes(in_ref[:, q], 0, 1) for q in range(pencil_count)]
    for index in range(groups):
        lines = []
        for z in range(index * group, (index + 1) * group):
            block = [turned[z] for turned in blocks]
            first = pltpu.roll(block[0] + block[2], LANES - y_local, 1)
            second = pltpu.roll(block[1] + block[3], LANES - y_local + part, 1)
            block.append(jnp.where(lane < part, first, second))
            lines.append(jnp.concatenate(block, axis=0).T[:y_local])
        lines = jnp.concatenate(lines, axis=0)
        field = product(split(lines), table, ((1,), (0,)))
        here = slice(index * group * y_local, (index + 1) * group * y_local)
        field_ref[here, :] = mean_ref[here, :] + field
        send(index).start()
    for index in range(groups):
        send(index).wait()


def whole():
    return pl.BlockSpec(memory_space=pltpu.VMEM)


def scalars():
    return pl.BlockSpec(memory_space=pltpu.SMEM)


def in_hbm(array):
    return pltpu.with_memory_space_constraint(array, pltpu.HBM)


def params(limit):
    return pltpu.CompilerParams(vmem_limit_bytes=limit * MIB)


def body(
    density_history, residual_history, occupancy_history, occupancy_residual, species, slot_count
):
    histories, z_local, y_local, x_length = residual_history.shape
    slab_count = lax.axis_size(SLAB)
    pencil_count = lax.axis_size("pencil")
    devices = slab_count * pencil_count
    y_length = y_local * pencil_count
    z_length = z_local * slab_count
    slots, entries = occupancy_residual.shape[1:]
    kx_local = x_length // slab_count
    rows = devices * z_local
    part = y_local // 2
    cell_total = float(z_length * y_length * x_length)
    x_order = (np.arange(slab_count)[None, :] * kx_local + np.arange(kx_local)[:, None]).reshape(-1)
    x_table = hartley(x_order, np.arange(x_length), x_length)
    y_tables = []
    for half in range(2):
        for kind in range(2):
            freq = 2 * np.arange(y_length // 2) + kind
            terms = [np.zeros((pencil_count // 2, LANES, 2, y_length // 2), bf16) for _ in range(2)]
            for q in range(pencil_count // 2):
                point = q * y_local + np.arange(y_local)
                whole_terms = hartley(point, freq, y_length)
                part_terms = hartley(point[half * part : (half + 1) * part], freq, y_length)
                for term, own, some in zip(terms, whole_terms, part_terms):
                    term[q, :y_local, 0] = own
                    term[q, y_local : y_local + part, 1] = some
            y_tables.append([term.reshape(-1, y_length) for term in terms])
    y_table = [np.stack(terms) for terms in zip(*y_tables)]
    z_half = np.arange(z_length // 2)
    z_table = [
        np.stack(terms)
        for terms in zip(
            hartley(2 * z_half, z_half, z_length),
            hartley(2 * z_half + 1, z_half, z_length),
        )
    ]
    place = jnp.stack([lax.axis_index(SLAB), lax.axis_index("pencil")]).astype(jnp.int32)
    place, species = lax.optimization_barrier((place, species))

    sums, held = pl.pallas_call(
        functools.partial(
            gram_kernel, cell_total=cell_total, block_total=100.0 * slots * devices
        ),
        in_specs=[scalars(), scalars(), pl.BlockSpec(memory_space=pltpu.HBM), whole()],
        out_specs=[whole(), whole()],
        out_shape=[
            jax.ShapeDtypeStruct((devices, LANES), f32),
            jax.ShapeDtypeStruct(residual_history.shape, f32),
        ],
        scratch_shapes=[
            pltpu.VMEM((len(pair_list(histories)), 8, x_length), f32),
            pltpu.SemaphoreType.DMA((z_local,)),
        ],
        compiler_params=params(16),
        name="gram",
    )(in_hbm(species), slot_count, in_hbm(residual_history), in_hbm(occupancy_residual))

    def exchange(array):
        return lax.all_to_all(
            array.reshape(devices, -1, LANES), SLAB_PENCIL, split_axis=0, concat_axis=0, tiled=True
        )

    sums = exchange(sums).reshape(devices, LANES)
    packed, weights = pl.pallas_call(
        functools.partial(mix_kernel, slab_count=slab_count),
        in_specs=[whole()] * 4,
        out_specs=[whole(), whole()],
        out_shape=[
            jax.ShapeDtypeStruct((slab_count, pencil_count, z_local, LANES), f32),
            jax.ShapeDtypeStruct((8, LANES), f32),
        ],
        scratch_shapes=[
            pltpu.VMEM((z_local * LANES, x_length), bf16),
            pltpu.VMEM((z_local * LANES, x_length), bf16),
        ],
        compiler_params=params(24),
        name="mix",
    )(sums, held, *x_table)
    moved = exchange(packed).reshape(slab_count, pencil_count, z_local, LANES)
    plane_in = pl.BlockSpec((histories, 1, y_local, x_length), lambda z: (0, z, 0, 0))
    mean, new_occupancy = pl.pallas_call(
        mean_kernel,
        grid=(z_local,),
        in_specs=[scalars(), scalars(), whole(), plane_in, whole(), whole()],
        out_specs=[
            pl.BlockSpec((1, y_local, x_length), lambda z: (z, 0, 0)),
            whole(),
        ],
        out_shape=[
            jax.ShapeDtypeStruct((z_local, y_local, x_length), f32),
            jax.ShapeDtypeStruct((slots, entries), f32),
        ],
        compiler_params=params(16),
        name="mean",
    )(species, slot_count, weights, density_history, occupancy_history, occupancy_residual)
    packed = pl.pallas_call(
        functools.partial(
            plane_kernel,
            x_length=x_length,
            y_length=y_length,
            z_length=z_length,
            scale=grid_mixing / cell_total,
        ),
        in_specs=[scalars()] + [whole()] * 5,
        out_specs=pl.BlockSpec(memory_space=pltpu.HBM),
        out_shape=jax.ShapeDtypeStruct((slab_count, pencil_count, z_local, LANES), f32),
        scratch_shapes=[
            pltpu.VMEM((slab_count, pencil_count, z_local, LANES), f32),
            pltpu.SemaphoreType.DMA((2 * pencil_count,)),
        ],
        compiler_params=params(32),
        name="plane",
    )(place, moved, *z_table, *y_table)
    moved = exchange(packed).reshape(slab_count, pencil_count, z_local, LANES)
    new_density = pl.pallas_call(
        functools.partial(
            x_inverse_kernel, slab_count=slab_count, pencil_count=pencil_count, z_local=z_local
        ),
        in_specs=[whole()] * 4,
        out_specs=pl.BlockSpec(memory_space=pltpu.HBM),
        out_shape=jax.ShapeDtypeStruct((z_local * y_local, x_length), f32),
        scratch_shapes=[
            pltpu.VMEM((z_local * y_local, x_length), f32),
            pltpu.SemaphoreType.DMA((2,)),
        ],
        compiler_params=params(24),
        name="x_inverse",
    )(moved, mean.reshape(z_local * y_local, x_length), *x_table)
    return (new_density.reshape(z_local, y_local, x_length), new_occupancy)


def solution(mesh):
    torus = Mesh(
        mesh.devices.reshape(8, 4, 2, mesh.shape["pencil"]),
        ("slab_0", "slab_1", "slab_2", "pencil"),
    )
    placed = (
        P(None, SLAB, "pencil", None),
        P(None, SLAB, "pencil", None),
        P(None, SLAB_PENCIL, None),
        P(None, SLAB_PENCIL, None),
        P(SLAB_PENCIL),
        P(SLAB_PENCIL),
    )
    return jax.shard_map(
        body,
        mesh=torus,
        in_specs=placed,
        out_specs=(P(SLAB, "pencil", None), P(SLAB_PENCIL, None)),
        check_vma=False,
    )
```

```python
import functools
import math

import jax
import jax.numpy as jnp
import numpy as np
from jax import lax
from jax.experimental import pallas as pl
from jax.experimental.pallas import tpu as pltpu
from jax.sharding import Mesh
from jax.sharding import PartitionSpec as P

ORBITALS = 18
SLAB = ("slab_0", "slab_1", "slab_2")
SLAB_PENCIL = ("slab_0", "slab_1", "slab_2", "pencil")

grid_mixing = 0.5
block_mixing = 0.5
kerker_wave = 6.0
species_orbitals = (18, 13, 8, 5)

f32 = jnp.float32
bf16 = jnp.bfloat16
LANES = 128
MIB = 1 << 20


def pair_list(histories):
    return [(i, j) for i in range(histories) for j in range(i, histories)]


def split(value):
    high = value.astype(bf16)
    return high, (value - high.astype(f32)).astype(bf16)


def product(left, right, dims):
    dot = functools.partial(
        lax.dot_general, dimension_numbers=(dims, ((), ())), preferred_element_type=f32
    )
    axis = 1 - dims[0][0]
    rows = left[0].shape[axis]
    both = dot(jnp.concatenate(left, axis=axis), right[0])
    return both[:rows] + (dot(left[0], right[1]) + both[rows:])


def hartley(rows, columns, length):
    angle = (np.outer(rows, columns) % length) * (2.0 * math.pi / length)
    table = np.cos(angle) + np.sin(angle)
    high = table.astype(bf16)
    low = (table - high.astype(np.float64)).astype(bf16)
    return high, low


def block_mask(species_ref, count_ref, slots, entries):
    row = lax.broadcasted_iota(jnp.int32, (slots, entries), 0)
    entry = lax.broadcasted_iota(jnp.int32, (slots, entries), 1)
    row_index = (entry * 3641) >> 16
    column_index = entry - ORBITALS * row_index
    limit = jnp.zeros((slots, entries), jnp.int32)
    for slot in range(slots):
        kind = species_ref[slot]
        number = jnp.int32(0)
        for index, orbital_number in enumerate(species_orbitals):
            number = jnp.where(kind == index, jnp.int32(orbital_number), number)
        number = jnp.where(slot < count_ref[0], number, jnp.int32(0))
        limit = jnp.where(row == slot, number, limit)
    return (row_index < limit) & (column_index < limit)


def gram_kernel(
    species_ref,
    count_ref,
    residual_ref,
    block_ref,
    out_ref,
    held_ref,
    acc_ref,
    arrived,
    *,
    cell_total,
    block_total,
):
    histories, planes, rows, width = residual_ref.shape
    pairs = pair_list(histories)

    def fetch(z):
        return pltpu.make_async_copy(residual_ref.at[:, z], held_ref.at[:, z], arrived.at[z])

    for z in range(planes):
        fetch(z).start()
    acc_ref[...] = jnp.zeros_like(acc_ref)
    _, slots, entries = block_ref.shape
    mask = block_mask(species_ref, count_ref, slots, entries)
    blocks = [jnp.where(mask, block_ref[i], 0.0) for i in range(histories)]
    lane = lax.broadcasted_iota(jnp.int32, (1, LANES), 1)
    line = jnp.zeros((1, LANES), f32)
    for k, (i, j) in enumerate(pairs):
        block_part = jnp.sum(blocks[i] * blocks[j], axis=(0, 1), keepdims=True) / block_total
        line = jnp.where(lane == k, block_part, line)

    def plane(z, carry):
        fetch(z).wait()
        for start in range(0, width, LANES):
            lanes = slice(start, min(start + LANES, width))
            accs = [acc_ref[k, :, lanes] for k in range(len(pairs))]
            for top in range(0, rows, 8):
                values = [held_ref[i, z, top : top + 8, lanes] for i in range(histories)]
                accs = [acc + values[i] * values[j] for acc, (i, j) in zip(accs, pairs)]
            for k, acc in enumerate(accs):
                acc_ref[k, :, lanes] = acc
        return carry

    lax.fori_loop(0, planes, plane, 0)
    for k in range(len(pairs)):
        grid_part = jnp.sum(acc_ref[k], axis=(0, 1), keepdims=True) / cell_total
        line = jnp.where(lane == k, line + grid_part, line)
    out_ref[...] = jnp.broadcast_to(line, out_ref.shape)


def mixing_weights(line, histories):
    lane = lax.broadcasted_iota(jnp.int32, (1, LANES), 1)
    entry = {}
    for k, (i, j) in enumerate(pair_list(histories)):
        entry[j, i] = jnp.sum(jnp.where(lane == k, line, 0.0), axis=1, keepdims=True)
    factor = {}
    inverse = {}
    work = dict(entry)
    for k in range(histories):
        inverse[k] = 1.0 / work[k, k]
        for i in range(k + 1, histories):
            factor[i, k] = work[i, k] * inverse[k]
        for i in range(k + 1, histories):
            for j in range(k + 1, i + 1):
                work[i, j] = work[i, j] - factor[i, k] * work[j, k]
    solved = [jnp.ones((1, 1), f32) for _ in range(histories)]
    for i in range(histories):
        for k in range(i):
            solved[i] = solved[i] - factor[i, k] * solved[k]
    solved = [value * inverse[i] for i, value in enumerate(solved)]
    for i in reversed(range(histories)):
        for k in range(i + 1, histories):
            solved[i] = solved[i] - factor[k, i] * solved[k]
    total = solved[0]
    for value in solved[1:]:
        total = total + value
    return [value / total for value in solved]


def mix_kernel(
    sums_ref, residual_ref, high_ref, low_ref, out_ref, weights_ref, mixed_high, mixed_low, *, slab_count
):
    histories, planes, rows, _ = residual_ref.shape
    line = jnp.sum(sums_ref[...], axis=0, keepdims=True)
    weights = mixing_weights(line, histories)
    for i, weight in enumerate(weights):
        weights_ref[i : i + 1, :] = jnp.broadcast_to(weight, (1, LANES))
    weights_ref[histories:, :] = jnp.zeros((8 - histories, LANES), f32)
    for z in range(planes):
        mixed = weights[0] * residual_ref[0, z]
        for i in range(1, histories):
            mixed = mixed + weights[i] * residual_ref[i, z]
        high, low = split(mixed)
        filler = jnp.zeros((LANES - rows, mixed.shape[1]), bf16)
        mixed_high[z * LANES : z * LANES + rows, :] = high
        mixed_high[z * LANES + rows : (z + 1) * LANES, :] = filler
        mixed_low[z * LANES : z * LANES + rows, :] = low
        mixed_low[z * LANES + rows : (z + 1) * LANES, :] = filler
    table = (high_ref[...], low_ref[...])
    result = product(table, (mixed_high[...], mixed_low[...]), ((1,), (1,)))
    own_planes = result.shape[0] // slab_count - 1
    part = rows // 2
    lane = lax.broadcasted_iota(jnp.int32, (slab_count, LANES), 1)
    here = (lane >= rows) & (lane < rows + part)
    shared = []
    for shift in (rows, rows - part):
        shared.append(
            [
                jnp.where(
                    here,
                    pltpu.roll(
                        result[own_planes * slab_count :, z * LANES : (z + 1) * LANES], shift, 1
                    ),
                    0.0,
                )
                for z in range(planes)
            ]
        )
    for own in range(own_planes):
        lines = [
            result[own * slab_count : (own + 1) * slab_count, z * LANES : (z + 1) * LANES]
            + shared[own // 2][z]
            for z in range(planes)
        ]
        out_ref[:, own] = jnp.swapaxes(jnp.stack(lines), 0, 1)


def plane_kernel(
    place_ref,
    in_ref,
    zh_ref,
    zl_ref,
    yh_ref,
    yl_ref,
    out_ref,
    made_ref,
    sent,
    *,
    x_length,
    y_length,
    z_length,
    scale,
):
    slab_count, pencil_count, z_local, _ = in_ref.shape
    z_half = z_length // 2
    y_half = y_length // 2
    s_half = slab_count // 2
    fold = pencil_count // 2 * LANES
    in_half = place_ref[1] // 2
    out_half = place_ref[1] % 2

    def gathered(first):
        return jnp.concatenate(
            [
                in_ref[first : first + s_half, q].reshape(z_half, LANES)
                for q in range(pencil_count)
            ],
            axis=1,
        )

    def z_table(kind):
        return (zh_ref[kind], zl_ref[kind])

    def y_table(half, kind):
        return (yh_ref[2 * half + kind], yl_ref[2 * half + kind])

    low, high = gathered(0), gathered(s_half)
    lines = jnp.concatenate(
        [
            product(z_table(0), split(low + high), ((1,), (0,))),
            product(z_table(1), split(low - high), ((1,), (0,))),
        ],
        axis=0,
    )
    folded = [lines[:, :fold] + lines[:, fold:], lines[:, :fold] - lines[:, fold:]]
    row = lax.broadcasted_iota(jnp.int32, (z_length, 1), 0)
    lane = lax.broadcasted_iota(jnp.int32, (1, y_length), 1)
    freq_z = jnp.where(row < z_half, 2 * row, 2 * row - (z_length - 1))
    first_x = place_ref[0] * (pencil_count + 1)
    freq_x = jnp.where(lane < y_half, first_x + place_ref[1], first_x + pencil_count)

    def squared(index, length):
        least = jnp.minimum(index, length - index).astype(f32)
        return least * least

    kept = []
    for kind in range(2):
        spectrum = product(split(folded[kind]), y_table(in_half, kind), ((1,), (0,)))
        freq_y = 2 * jnp.where(lane < y_half, lane, lane - y_half) + kind
        square = squared(freq_z, z_length) + (
            squared(freq_y, y_length) + squared(freq_x, x_length)
        )
        kept.append(spectrum * (square / (square + kerker_wave * kerker_wave) * scale))
    parts = []
    for rows in (slice(0, z_half), slice(z_half, z_length)):
        results = [
            product(split(kept[kind][rows]), y_table(out_half, kind), ((1,), (1,)))
            for kind in range(2)
        ]
        parts.append(split(jnp.concatenate([results[0] + results[1], results[0] - results[1]], axis=1)))
    sends = []
    for q in range(pencil_count):
        for first in (0, s_half):
            here = pl.ds(first, s_half)
            sends.append(
                pltpu.make_async_copy(
                    made_ref.at[here, q], out_ref.at[here, q], sent.at[len(sends)]
                )
            )
    even = product(z_table(0), parts[0], ((1,), (0,)))
    odd = product(z_table(1), parts[1], ((0,), (0,)))
    low, high = even + odd, even - odd
    for q in range(pencil_count):
        columns = slice(q * LANES, (q + 1) * LANES)
        made_ref[:s_half, q] = low[:, columns].reshape(s_half, z_local, LANES)
        sends[2 * q].start()
        made_ref[s_half:, q] = high[:, columns].reshape(s_half, z_local, LANES)
        sends[2 * q + 1].start()
    for send in sends:
        send.wait()


def mean_kernel(
    species_ref, count_ref, weights_ref, density_ref, block_ref, block_residual_ref, out_ref, out_block_ref
):
    step = pl.program_id(0)
    histories = density_ref.shape[0]
    weights = [weights_ref[i : i + 1, 0:1] for i in range(histories)]
    mean = weights[0] * density_ref[0, 0]
    for i in range(1, histories):
        mean = mean + weights[i] * density_ref[i, 0]
    out_ref[0] = mean

    @pl.when(step == 0)
    def _():
        _, slots, entries = block_ref.shape
        mask = block_mask(species_ref, count_ref, slots, entries)
        total = weights[0] * (block_ref[0] + block_mixing * block_residual_ref[0])
        for i in range(1, histories):
            total = total + weights[i] * (block_ref[i] + block_mixing * block_residual_ref[i])
        out_block_ref[...] = jnp.where(mask, total, 0.0)


def x_inverse_kernel(
    in_ref,
    mean_ref,
    high_ref,
    low_ref,
    out_ref,
    field_ref,
    sent,
    *,
    slab_count,
    pencil_count,
    z_local,
):
    rows, x_length = mean_ref.shape
    y_local = rows // z_local
    part = y_local // 2
    table = (high_ref[...], low_ref[...])
    lane = lax.broadcasted_iota(jnp.int32, (slab_count, LANES), 1)
    groups = sent.shape[0]
    group = z_local // groups

    def send(index):
        here = pl.ds(index * group * y_local, group * y_local)
        return pltpu.make_async_copy(field_ref.at[here], out_ref.at[here], sent.at[index])

    blocks = [jnp.swapaxes(in_ref[:, q], 0, 1) for q in range(pencil_count)]
    for index in range(groups):
        lines = []
        for z in range(index * group, (index + 1) * group):
            block = [turned[z] for turned in blocks]
            first = pltpu.roll(block[0] + block[2], LANES - y_local, 1)
            second = pltpu.roll(block[1] + block[3], LANES - y_local + part, 1)
            block.append(jnp.where(lane < part, first, second))
            lines.append(jnp.concatenate(block, axis=0).T[:y_local])
        lines = jnp.concatenate(lines, axis=0)
        field = product(split(lines), table, ((1,), (0,)))
        here = slice(index * group * y_local, (index + 1) * group * y_local)
        field_ref[here, :] = mean_ref[here, :] + field
        send(index).start()
    for index in range(groups):
        send(index).wait()


def whole():
    return pl.BlockSpec(memory_space=pltpu.VMEM)


def scalars():
    return pl.BlockSpec(memory_space=pltpu.SMEM)


def in_hbm(array):
    return pltpu.with_memory_space_constraint(array, pltpu.HBM)


def params(limit):
    return pltpu.CompilerParams(vmem_limit_bytes=limit * MIB)


def body(
    density_history, residual_history, occupancy_history, occupancy_residual, species, slot_count
):
    histories, z_local, y_local, x_length = residual_history.shape
    slab_count = lax.axis_size(SLAB)
    pencil_count = lax.axis_size("pencil")
    devices = slab_count * pencil_count
    y_length = y_local * pencil_count
    z_length = z_local * slab_count
    slots, entries = occupancy_residual.shape[1:]
    kx_local = x_length // slab_count
    rows = devices * z_local
    part = y_local // 2
    cell_total = float(z_length * y_length * x_length)
    x_order = (np.arange(slab_count)[None, :] * kx_local + np.arange(kx_local)[:, None]).reshape(-1)
    x_table = hartley(x_order, np.arange(x_length), x_length)
    y_tables = []
    for half in range(2):
        for kind in range(2):
            freq = 2 * np.arange(y_length // 2) + kind
            terms = [np.zeros((pencil_count // 2, LANES, 2, y_length // 2), bf16) for _ in range(2)]
            for q in range(pencil_count // 2):
                point = q * y_local + np.arange(y_local)
                whole_terms = hartley(point, freq, y_length)
                part_terms = hartley(point[half * part : (half + 1) * part], freq, y_length)
                for term, own, some in zip(terms, whole_terms, part_terms):
                    term[q, :y_local, 0] = own
                    term[q, y_local : y_local + part, 1] = some
            y_tables.append([term.reshape(-1, y_length) for term in terms])
    y_table = [np.stack(terms) for terms in zip(*y_tables)]
    z_half = np.arange(z_length // 2)
    z_table = [
        np.stack(terms)
        for terms in zip(
            hartley(2 * z_half, z_half, z_length),
            hartley(2 * z_half + 1, z_half, z_length),
        )
    ]
    place = jnp.stack([lax.axis_index(SLAB), lax.axis_index("pencil")]).astype(jnp.int32)
    place, species = lax.optimization_barrier((place, species))

    sums, held = pl.pallas_call(
        functools.partial(
            gram_kernel, cell_total=cell_total, block_total=100.0 * slots * devices
        ),
        in_specs=[scalars(), scalars(), pl.BlockSpec(memory_space=pltpu.HBM), whole()],
        out_specs=[whole(), whole()],
        out_shape=[
            jax.ShapeDtypeStruct((devices, LANES), f32),
            jax.ShapeDtypeStruct(residual_history.shape, f32),
        ],
        scratch_shapes=[
            pltpu.VMEM((len(pair_list(histories)), 8, x_length), f32),
            pltpu.SemaphoreType.DMA((z_local,)),
        ],
        compiler_params=params(16),
        name="gram",
    )(in_hbm(species), slot_count, in_hbm(residual_history), in_hbm(occupancy_residual))

    def exchange(array):
        return lax.all_to_all(
            array.reshape(devices, -1, LANES), SLAB_PENCIL, split_axis=0, concat_axis=0, tiled=True
        )

    sums = exchange(sums).reshape(devices, LANES)
    packed, weights = pl.pallas_call(
        functools.partial(mix_kernel, slab_count=slab_count),
        in_specs=[whole()] * 4,
        out_specs=[whole(), whole()],
        out_shape=[
            jax.ShapeDtypeStruct((slab_count, pencil_count, z_local, LANES), f32),
            jax.ShapeDtypeStruct((8, LANES), f32),
        ],
        scratch_shapes=[
            pltpu.VMEM((z_local * LANES, x_length), bf16),
            pltpu.VMEM((z_local * LANES, x_length), bf16),
        ],
        compiler_params=params(24),
        name="mix",
    )(sums, held, *x_table)
    moved = exchange(packed).reshape(slab_count, pencil_count, z_local, LANES)
    plane_in = pl.BlockSpec((histories, 1, y_local, x_length), lambda z: (0, z, 0, 0))
    mean, new_occupancy = pl.pallas_call(
        mean_kernel,
        grid=(z_local,),
        in_specs=[scalars(), scalars(), whole(), plane_in, whole(), whole()],
        out_specs=[
            pl.BlockSpec((1, y_local, x_length), lambda z: (z, 0, 0)),
            whole(),
        ],
        out_shape=[
            jax.ShapeDtypeStruct((z_local, y_local, x_length), f32),
            jax.ShapeDtypeStruct((slots, entries), f32),
        ],
        compiler_params=params(16),
        name="mean",
    )(species, slot_count, weights, density_history, occupancy_history, occupancy_residual)
    packed = pl.pallas_call(
        functools.partial(
            plane_kernel,
            x_length=x_length,
            y_length=y_length,
            z_length=z_length,
            scale=grid_mixing / cell_total,
        ),
        in_specs=[scalars()] + [whole()] * 5,
        out_specs=pl.BlockSpec(memory_space=pltpu.HBM),
        out_shape=jax.ShapeDtypeStruct((slab_count, pencil_count, z_local, LANES), f32),
        scratch_shapes=[
            pltpu.VMEM((slab_count, pencil_count, z_local, LANES), f32),
            pltpu.SemaphoreType.DMA((2 * pencil_count,)),
        ],
        compiler_params=params(32),
        name="plane",
    )(place, moved, *z_table, *y_table)
    moved = exchange(packed).reshape(slab_count, pencil_count, z_local, LANES)
    new_density = pl.pallas_call(
        functools.partial(
            x_inverse_kernel, slab_count=slab_count, pencil_count=pencil_count, z_local=z_local
        ),
        in_specs=[whole()] * 4,
        out_specs=pl.BlockSpec(memory_space=pltpu.HBM),
        out_shape=jax.ShapeDtypeStruct((z_local * y_local, x_length), f32),
        scratch_shapes=[
            pltpu.VMEM((z_local * y_local, x_length), f32),
            pltpu.SemaphoreType.DMA((2,)),
        ],
        compiler_params=params(24),
        name="x_inverse",
    )(moved, mean.reshape(z_local * y_local, x_length), *x_table)
    return (new_density.reshape(z_local, y_local, x_length), new_occupancy)


def solution(mesh):
    torus = Mesh(
        mesh.devices.reshape(8, 4, 2, mesh.shape["pencil"]),
        ("slab_0", "slab_1", "slab_2", "pencil"),
    )
    placed = (
        P(None, SLAB, "pencil", None),
        P(None, SLAB, "pencil", None),
        P(None, SLAB_PENCIL, None),
        P(None, SLAB_PENCIL, None),
        P(SLAB_PENCIL),
        P(SLAB_PENCIL),
    )
    return jax.shard_map(
        body,
        mesh=torus,
        in_specs=placed,
        out_specs=(P(SLAB, "pencil", None), P(SLAB_PENCIL, None)),
        check_vma=False,
    )
```

```python
import functools
import math

import jax
import jax.numpy as jnp
import numpy as np
from jax import lax
from jax.experimental import pallas as pl
from jax.experimental.pallas import tpu as pltpu
from jax.sharding import Mesh
from jax.sharding import PartitionSpec as P

ORBITALS = 18
SLAB = ("slab_0", "slab_1", "slab_2")
SLAB_PENCIL = ("slab_0", "slab_1", "slab_2", "pencil")

grid_mixing = 0.5
block_mixing = 0.5
kerker_wave = 6.0
species_orbitals = (18, 13, 8, 5)

f32 = jnp.float32
bf16 = jnp.bfloat16
LANES = 128
MIB = 1 << 20


def pair_list(histories):
    return [(i, j) for i in range(histories) for j in range(i, histories)]


def split(value):
    high = value.astype(bf16)
    return high, (value - high.astype(f32)).astype(bf16)


def product(left, right, dims):
    dot = functools.partial(
        lax.dot_general, dimension_numbers=(dims, ((), ())), preferred_element_type=f32
    )
    axis = 1 - dims[0][0]
    rows = left[0].shape[axis]
    both = dot(jnp.concatenate(left, axis=axis), right[0])
    return both[:rows] + (dot(left[0], right[1]) + both[rows:])


def hartley(rows, columns, length):
    angle = (np.outer(rows, columns) % length) * (2.0 * math.pi / length)
    table = np.cos(angle) + np.sin(angle)
    high = table.astype(bf16)
    low = (table - high.astype(np.float64)).astype(bf16)
    return high, low


def block_mask(species_ref, count_ref, slots, entries):
    row = lax.broadcasted_iota(jnp.int32, (slots, entries), 0)
    entry = lax.broadcasted_iota(jnp.int32, (slots, entries), 1)
    row_index = (entry * 3641) >> 16
    column_index = entry - ORBITALS * row_index
    limit = jnp.zeros((slots, entries), jnp.int32)
    for slot in range(slots):
        kind = species_ref[slot]
        number = jnp.int32(0)
        for index, orbital_number in enumerate(species_orbitals):
            number = jnp.where(kind == index, jnp.int32(orbital_number), number)
        number = jnp.where(slot < count_ref[0], number, jnp.int32(0))
        limit = jnp.where(row == slot, number, limit)
    return (row_index < limit) & (column_index < limit)


def gram_kernel(
    species_source,
    count_ref,
    residual_ref,
    block_source,
    out_ref,
    held_ref,
    acc_ref,
    species_ref,
    block_ref,
    arrived,
    small_arrived,
    *,
    cell_total,
    block_total,
):
    histories, planes, rows, width = residual_ref.shape
    pairs = pair_list(histories)

    def fetch(z):
        return pltpu.make_async_copy(residual_ref.at[:, z], held_ref.at[:, z], arrived.at[z])

    small = [
        pltpu.make_async_copy(source, target, small_arrived.at[index])
        for index, (source, target) in enumerate(
            (
                (species_source, species_ref),
                (block_source, block_ref),
            )
        )
    ]
    for copy in small:
        copy.start()
    for z in range(planes):
        fetch(z).start()
    acc_ref[...] = jnp.zeros_like(acc_ref)
    for copy in small:
        copy.wait()
    _, slots, entries = block_ref.shape
    mask = block_mask(species_ref, count_ref, slots, entries)
    blocks = [jnp.where(mask, block_ref[i], 0.0) for i in range(histories)]
    lane = lax.broadcasted_iota(jnp.int32, (1, LANES), 1)
    line = jnp.zeros((1, LANES), f32)
    for k, (i, j) in enumerate(pairs):
        block_part = jnp.sum(blocks[i] * blocks[j], axis=(0, 1), keepdims=True) / block_total
        line = jnp.where(lane == k, block_part, line)

    def plane(z, carry):
        fetch(z).wait()
        body_width = width // LANES * LANES
        for start in range(0, body_width, LANES):
            lanes = slice(start, start + LANES)
            accs = [acc_ref[k, :, lanes] for k in range(len(pairs))]
            for top in range(0, rows, 8):
                values = [held_ref[i, z, top : top + 8, lanes] for i in range(histories)]
                accs = [acc + values[i] * values[j] for acc, (i, j) in zip(accs, pairs)]
            for k, acc in enumerate(accs):
                acc_ref[k, :, lanes] = acc
        lanes = slice(body_width, width)
        accs = [acc_ref[k, :, body_width:] for k in range(len(pairs))]
        for top in range(0, rows, 16):
            values = [
                jnp.concatenate(
                    [held_ref[i, z, top : top + 8, lanes], held_ref[i, z, top + 8 : top + 16, lanes]],
                    axis=1,
                )
                for i in range(histories)
            ]
            accs = [acc + values[i] * values[j] for acc, (i, j) in zip(accs, pairs)]
        for k, acc in enumerate(accs):
            acc_ref[k, :, body_width:] = acc
        return carry

    lax.fori_loop(0, planes, plane, 0)
    for k in range(len(pairs)):
        grid_part = jnp.sum(acc_ref[k], axis=(0, 1), keepdims=True) / cell_total
        line = jnp.where(lane == k, line + grid_part, line)
    out_ref[...] = jnp.broadcast_to(line, out_ref.shape)


def mixing_weights(line, histories):
    lane = lax.broadcasted_iota(jnp.int32, (1, LANES), 1)
    entry = {}
    for k, (i, j) in enumerate(pair_list(histories)):
        entry[j, i] = jnp.sum(jnp.where(lane == k, line, 0.0), axis=1, keepdims=True)
    factor = {}
    inverse = {}
    work = dict(entry)
    for k in range(histories):
        inverse[k] = 1.0 / work[k, k]
        for i in range(k + 1, histories):
            factor[i, k] = work[i, k] * inverse[k]
        for i in range(k + 1, histories):
            for j in range(k + 1, i + 1):
                work[i, j] = work[i, j] - factor[i, k] * work[j, k]
    solved = [jnp.ones((1, 1), f32) for _ in range(histories)]
    for i in range(histories):
        for k in range(i):
            solved[i] = solved[i] - factor[i, k] * solved[k]
    solved = [value * inverse[i] for i, value in enumerate(solved)]
    for i in reversed(range(histories)):
        for k in range(i + 1, histories):
            solved[i] = solved[i] - factor[k, i] * solved[k]
    total = solved[0]
    for value in solved[1:]:
        total = total + value
    return [value / total for value in solved]


def mix_kernel(
    sums_ref, residual_ref, high_ref, low_ref, out_ref, weights_ref, mixed_high, mixed_low, *, slab_count
):
    histories, planes, rows, _ = residual_ref.shape
    line = jnp.sum(sums_ref[...], axis=0, keepdims=True)
    weights = mixing_weights(line, histories)
    for i, weight in enumerate(weights):
        weights_ref[i : i + 1, :] = jnp.broadcast_to(weight, (1, LANES))
    weights_ref[histories:, :] = jnp.zeros((8 - histories, LANES), f32)
    for z in range(planes):
        mixed = weights[0] * residual_ref[0, z]
        for i in range(1, histories):
            mixed = mixed + weights[i] * residual_ref[i, z]
        high, low = split(mixed)
        filler = jnp.zeros((LANES - rows, mixed.shape[1]), bf16)
        mixed_high[z * LANES : z * LANES + rows, :] = high
        mixed_high[z * LANES + rows : (z + 1) * LANES, :] = filler
        mixed_low[z * LANES : z * LANES + rows, :] = low
        mixed_low[z * LANES + rows : (z + 1) * LANES, :] = filler
    table = (high_ref[...], low_ref[...])
    result = product(table, (mixed_high[...], mixed_low[...]), ((1,), (1,)))
    own_planes = result.shape[0] // slab_count - 1
    part = rows // 2
    lane = lax.broadcasted_iota(jnp.int32, (slab_count, LANES), 1)
    here = (lane >= rows) & (lane < rows + part)
    shared = []
    for shift in (rows, rows - part):
        shared.append(
            [
                jnp.where(
                    here,
                    pltpu.roll(
                        result[own_planes * slab_count :, z * LANES : (z + 1) * LANES], shift, 1
                    ),
                    0.0,
                )
                for z in range(planes)
            ]
        )
    for own in range(own_planes):
        lines = [
            result[own * slab_count : (own + 1) * slab_count, z * LANES : (z + 1) * LANES]
            + shared[own // 2][z]
            for z in range(planes)
        ]
        out_ref[:, own] = jnp.swapaxes(jnp.stack(lines), 0, 1)


def plane_kernel(
    place_ref,
    in_ref,
    zh_ref,
    zl_ref,
    yh_ref,
    yl_ref,
    out_ref,
    made_ref,
    sent,
    *,
    x_length,
    y_length,
    z_length,
    scale,
):
    slab_count, pencil_count, z_local, _ = in_ref.shape
    z_half = z_length // 2
    y_half = y_length // 2
    s_half = slab_count // 2
    fold = pencil_count // 2 * LANES
    in_half = place_ref[1] // 2
    out_half = place_ref[1] % 2

    def gathered(first):
        return jnp.concatenate(
            [
                in_ref[first : first + s_half, q].reshape(z_half, LANES)
                for q in range(pencil_count)
            ],
            axis=1,
        )

    def z_table(kind):
        return (zh_ref[kind], zl_ref[kind])

    def y_table(half, kind):
        return (yh_ref[2 * half + kind], yl_ref[2 * half + kind])

    low, high = gathered(0), gathered(s_half)
    lines = jnp.concatenate(
        [
            product(z_table(0), split(low + high), ((1,), (0,))),
            product(z_table(1), split(low - high), ((1,), (0,))),
        ],
        axis=0,
    )
    folded = [lines[:, :fold] + lines[:, fold:], lines[:, :fold] - lines[:, fold:]]
    row = lax.broadcasted_iota(jnp.int32, (z_length, 1), 0)
    lane = lax.broadcasted_iota(jnp.int32, (1, y_length), 1)
    freq_z = jnp.where(row < z_half, 2 * row, 2 * row - (z_length - 1))
    first_x = place_ref[0] * (pencil_count + 1)
    freq_x = jnp.where(lane < y_half, first_x + place_ref[1], first_x + pencil_count)

    def squared(index, length):
        least = jnp.minimum(index, length - index).astype(f32)
        return least * least

    kept = []
    for kind in range(2):
        spectrum = product(split(folded[kind]), y_table(in_half, kind), ((1,), (0,)))
        freq_y = 2 * jnp.where(lane < y_half, lane, lane - y_half) + kind
        square = squared(freq_z, z_length) + (
            squared(freq_y, y_length) + squared(freq_x, x_length)
        )
        kept.append(spectrum * (square / (square + kerker_wave * kerker_wave) * scale))
    parts = []
    for rows in (slice(0, z_half), slice(z_half, z_length)):
        results = [
            product(split(kept[kind][rows]), y_table(out_half, kind), ((1,), (1,)))
            for kind in range(2)
        ]
        parts.append(split(jnp.concatenate([results[0] + results[1], results[0] - results[1]], axis=1)))
    sends = []
    for q in range(pencil_count):
        for first in (0, s_half):
            here = pl.ds(first, s_half)
            sends.append(
                pltpu.make_async_copy(
                    made_ref.at[here, q], out_ref.at[here, q], sent.at[len(sends)]
                )
            )
    even = product(z_table(0), parts[0], ((1,), (0,)))
    odd = product(z_table(1), parts[1], ((0,), (0,)))
    low, high = even + odd, even - odd
    for q in range(pencil_count):
        columns = slice(q * LANES, (q + 1) * LANES)
        made_ref[:s_half, q] = low[:, columns].reshape(s_half, z_local, LANES)
        sends[2 * q].start()
        made_ref[s_half:, q] = high[:, columns].reshape(s_half, z_local, LANES)
        sends[2 * q + 1].start()
    for send in sends:
        send.wait()


def mean_kernel(
    species_ref, count_ref, weights_ref, density_ref, block_ref, block_residual_ref, out_ref, out_block_ref
):
    step = pl.program_id(0)
    histories = density_ref.shape[0]
    weights = [weights_ref[i : i + 1, 0:1] for i in range(histories)]
    mean = weights[0] * density_ref[0, 0]
    for i in range(1, histories):
        mean = mean + weights[i] * density_ref[i, 0]
    out_ref[0] = mean

    @pl.when(step == 0)
    def _():
        _, slots, entries = block_ref.shape
        mask = block_mask(species_ref, count_ref, slots, entries)
        total = weights[0] * (block_ref[0] + block_mixing * block_residual_ref[0])
        for i in range(1, histories):
            total = total + weights[i] * (block_ref[i] + block_mixing * block_residual_ref[i])
        out_block_ref[...] = jnp.where(mask, total, 0.0)


def x_inverse_kernel(
    in_ref,
    mean_ref,
    high_ref,
    low_ref,
    out_ref,
    field_ref,
    sent,
    *,
    slab_count,
    pencil_count,
    z_local,
):
    rows, x_length = mean_ref.shape
    y_local = rows // z_local
    part = y_local // 2
    table = (high_ref[...], low_ref[...])
    lane = lax.broadcasted_iota(jnp.int32, (slab_count, LANES), 1)
    groups = sent.shape[0]
    group = z_local // groups

    def send(index):
        here = pl.ds(index * group * y_local, group * y_local)
        return pltpu.make_async_copy(field_ref.at[here], out_ref.at[here], sent.at[index])

    blocks = [jnp.swapaxes(in_ref[:, q], 0, 1) for q in range(pencil_count)]
    for index in range(groups):
        lines = []
        for z in range(index * group, (index + 1) * group):
            block = [turned[z] for turned in blocks]
            first = pltpu.roll(block[0] + block[2], LANES - y_local, 1)
            second = pltpu.roll(block[1] + block[3], LANES - y_local + part, 1)
            block.append(jnp.where(lane < part, first, second))
            lines.append(jnp.concatenate(block, axis=0).T[:y_local])
        lines = jnp.concatenate(lines, axis=0)
        field = product(split(lines), table, ((1,), (0,)))
        here = slice(index * group * y_local, (index + 1) * group * y_local)
        field_ref[here, :] = mean_ref[here, :] + field
        send(index).start()
    for index in range(groups):
        send(index).wait()


def whole():
    return pl.BlockSpec(memory_space=pltpu.VMEM)


def scalars():
    return pl.BlockSpec(memory_space=pltpu.SMEM)


def in_hbm(array):
    return pltpu.with_memory_space_constraint(array, pltpu.HBM)


def params(limit):
    return pltpu.CompilerParams(vmem_limit_bytes=limit * MIB)


def body(
    density_history, residual_history, occupancy_history, occupancy_residual, species, slot_count
):
    histories, z_local, y_local, x_length = residual_history.shape
    slab_count = lax.axis_size(SLAB)
    pencil_count = lax.axis_size("pencil")
    devices = slab_count * pencil_count
    y_length = y_local * pencil_count
    z_length = z_local * slab_count
    slots, entries = occupancy_residual.shape[1:]
    kx_local = x_length // slab_count
    rows = devices * z_local
    part = y_local // 2
    cell_total = float(z_length * y_length * x_length)
    x_order = (np.arange(slab_count)[None, :] * kx_local + np.arange(kx_local)[:, None]).reshape(-1)
    x_table = hartley(x_order, np.arange(x_length), x_length)
    y_tables = []
    for half in range(2):
        for kind in range(2):
            freq = 2 * np.arange(y_length // 2) + kind
            terms = [np.zeros((pencil_count // 2, LANES, 2, y_length // 2), bf16) for _ in range(2)]
            for q in range(pencil_count // 2):
                point = q * y_local + np.arange(y_local)
                whole_terms = hartley(point, freq, y_length)
                part_terms = hartley(point[half * part : (half + 1) * part], freq, y_length)
                for term, own, some in zip(terms, whole_terms, part_terms):
                    term[q, :y_local, 0] = own
                    term[q, y_local : y_local + part, 1] = some
            y_tables.append([term.reshape(-1, y_length) for term in terms])
    y_table = [np.stack(terms) for terms in zip(*y_tables)]
    z_half = np.arange(z_length // 2)
    z_table = [
        np.stack(terms)
        for terms in zip(
            hartley(2 * z_half, z_half, z_length),
            hartley(2 * z_half + 1, z_half, z_length),
        )
    ]
    place = jnp.stack([lax.axis_index(SLAB), lax.axis_index("pencil")]).astype(jnp.int32)
    place, species = lax.optimization_barrier((place, species))

    in_place = pl.BlockSpec(memory_space=pltpu.HBM)
    sums, held = pl.pallas_call(
        functools.partial(
            gram_kernel, cell_total=cell_total, block_total=100.0 * slots * devices
        ),
        in_specs=[in_place, scalars(), in_place, in_place],
        out_specs=[whole(), whole()],
        out_shape=[
            jax.ShapeDtypeStruct((devices, LANES), f32),
            jax.ShapeDtypeStruct(residual_history.shape, f32),
        ],
        scratch_shapes=[
            pltpu.VMEM((len(pair_list(histories)), 8, -(-x_length // LANES) * LANES), f32),
            pltpu.SMEM(species.shape, jnp.int32),
            pltpu.VMEM(occupancy_residual.shape, f32),
            pltpu.SemaphoreType.DMA((z_local,)),
            pltpu.SemaphoreType.DMA((2,)),
        ],
        compiler_params=params(16),
        name="gram",
    )(in_hbm(species), slot_count, in_hbm(residual_history), in_hbm(occupancy_residual))

    def exchange(array):
        return lax.all_to_all(
            array.reshape(devices, -1, LANES), SLAB_PENCIL, split_axis=0, concat_axis=0, tiled=True
        )

    sums = exchange(sums).reshape(devices, LANES)
    packed, weights = pl.pallas_call(
        functools.partial(mix_kernel, slab_count=slab_count),
        in_specs=[whole()] * 4,
        out_specs=[whole(), whole()],
        out_shape=[
            jax.ShapeDtypeStruct((slab_count, pencil_count, z_local, LANES), f32),
            jax.ShapeDtypeStruct((8, LANES), f32),
        ],
        scratch_shapes=[
            pltpu.VMEM((z_local * LANES, x_length), bf16),
            pltpu.VMEM((z_local * LANES, x_length), bf16),
        ],
        compiler_params=params(24),
        name="mix",
    )(sums, held, *x_table)
    moved = exchange(packed).reshape(slab_count, pencil_count, z_local, LANES)
    plane_in = pl.BlockSpec((histories, 1, y_local, x_length), lambda z: (0, z, 0, 0))
    mean, new_occupancy = pl.pallas_call(
        mean_kernel,
        grid=(z_local,),
        in_specs=[scalars(), scalars(), whole(), plane_in, whole(), whole()],
        out_specs=[
            pl.BlockSpec((1, y_local, x_length), lambda z: (z, 0, 0)),
            whole(),
        ],
        out_shape=[
            jax.ShapeDtypeStruct((z_local, y_local, x_length), f32),
            jax.ShapeDtypeStruct((slots, entries), f32),
        ],
        compiler_params=params(16),
        name="mean",
    )(species, slot_count, weights, density_history, occupancy_history, occupancy_residual)
    packed = pl.pallas_call(
        functools.partial(
            plane_kernel,
            x_length=x_length,
            y_length=y_length,
            z_length=z_length,
            scale=grid_mixing / cell_total,
        ),
        in_specs=[scalars()] + [whole()] * 5,
        out_specs=pl.BlockSpec(memory_space=pltpu.HBM),
        out_shape=jax.ShapeDtypeStruct((slab_count, pencil_count, z_local, LANES), f32),
        scratch_shapes=[
            pltpu.VMEM((slab_count, pencil_count, z_local, LANES), f32),
            pltpu.SemaphoreType.DMA((2 * pencil_count,)),
        ],
        compiler_params=params(32),
        name="plane",
    )(place, moved, *z_table, *y_table)
    moved = exchange(packed).reshape(slab_count, pencil_count, z_local, LANES)
    new_density = pl.pallas_call(
        functools.partial(
            x_inverse_kernel, slab_count=slab_count, pencil_count=pencil_count, z_local=z_local
        ),
        in_specs=[whole()] * 4,
        out_specs=pl.BlockSpec(memory_space=pltpu.HBM),
        out_shape=jax.ShapeDtypeStruct((z_local * y_local, x_length), f32),
        scratch_shapes=[
            pltpu.VMEM((z_local * y_local, x_length), f32),
            pltpu.SemaphoreType.DMA((2,)),
        ],
        compiler_params=params(24),
        name="x_inverse",
    )(moved, mean.reshape(z_local * y_local, x_length), *x_table)
    return (new_density.reshape(z_local, y_local, x_length), new_occupancy)


def solution(mesh):
    torus = Mesh(
        mesh.devices.reshape(8, 4, 2, mesh.shape["pencil"]),
        ("slab_0", "slab_1", "slab_2", "pencil"),
    )
    placed = (
        P(None, SLAB, "pencil", None),
        P(None, SLAB, "pencil", None),
        P(None, SLAB_PENCIL, None),
        P(None, SLAB_PENCIL, None),
        P(SLAB_PENCIL),
        P(SLAB_PENCIL),
    )
    return jax.shard_map(
        body,
        mesh=torus,
        in_specs=placed,
        out_specs=(P(SLAB, "pencil", None), P(SLAB_PENCIL, None)),
        check_vma=False,
    )
```

```python
import functools
import math

import jax
import jax.numpy as jnp
import numpy as np
from jax import lax
from jax.experimental import pallas as pl
from jax.experimental.pallas import tpu as pltpu
from jax.sharding import Mesh
from jax.sharding import PartitionSpec as P

ORBITALS = 18
SLAB = ("slab_0", "slab_1", "slab_2")
SLAB_PENCIL = ("slab_0", "slab_1", "slab_2", "pencil")

grid_mixing = 0.5
block_mixing = 0.5
kerker_wave = 6.0
species_orbitals = (18, 13, 8, 5)

f32 = jnp.float32
bf16 = jnp.bfloat16
LANES = 128
MIB = 1 << 20


def pair_list(histories):
    return [(i, j) for i in range(histories) for j in range(i, histories)]


def split(value):
    high = value.astype(bf16)
    return high, (value - high.astype(f32)).astype(bf16)


def product(left, right, dims):
    dot = functools.partial(
        lax.dot_general, dimension_numbers=(dims, ((), ())), preferred_element_type=f32
    )
    axis = 1 - dims[0][0]
    rows = left[0].shape[axis]
    both = dot(jnp.concatenate(left, axis=axis), right[0])
    return both[:rows] + (dot(left[0], right[1]) + both[rows:])


def hartley(rows, columns, length):
    angle = (np.outer(rows, columns) % length) * (2.0 * math.pi / length)
    table = np.cos(angle) + np.sin(angle)
    high = table.astype(bf16)
    low = (table - high.astype(np.float64)).astype(bf16)
    return high, low


def block_mask(species_ref, count_ref, slots, entries):
    row = lax.broadcasted_iota(jnp.int32, (slots, entries), 0)
    entry = lax.broadcasted_iota(jnp.int32, (slots, entries), 1)
    row_index = (entry * 3641) >> 16
    column_index = entry - ORBITALS * row_index
    limit = jnp.zeros((slots, entries), jnp.int32)
    for slot in range(slots):
        kind = species_ref[slot]
        number = jnp.int32(0)
        for index, orbital_number in enumerate(species_orbitals):
            number = jnp.where(kind == index, jnp.int32(orbital_number), number)
        number = jnp.where(slot < count_ref[0], number, jnp.int32(0))
        limit = jnp.where(row == slot, number, limit)
    return (row_index < limit) & (column_index < limit)


def gram_kernel(
    species_ref,
    count_ref,
    residual_ref,
    block_ref,
    out_ref,
    held_ref,
    acc_ref,
    arrived,
    *,
    cell_total,
    block_total,
):
    histories, planes, rows, width = residual_ref.shape
    pairs = pair_list(histories)

    def fetch(z):
        return pltpu.make_async_copy(residual_ref.at[:, z], held_ref.at[:, z], arrived.at[z])

    for z in range(planes):
        fetch(z).start()
    acc_ref[...] = jnp.zeros_like(acc_ref)
    _, slots, entries = block_ref.shape
    mask = block_mask(species_ref, count_ref, slots, entries)
    blocks = [jnp.where(mask, block_ref[i], 0.0) for i in range(histories)]
    lane = lax.broadcasted_iota(jnp.int32, (1, LANES), 1)
    line = jnp.zeros((1, LANES), f32)
    for k, (i, j) in enumerate(pairs):
        block_part = jnp.sum(blocks[i] * blocks[j], axis=(0, 1), keepdims=True) / block_total
        line = jnp.where(lane == k, block_part, line)

    def plane(z, carry):
        fetch(z).wait()
        body_width = width // LANES * LANES
        for start in range(0, body_width, LANES):
            lanes = slice(start, start + LANES)
            accs = [acc_ref[k, :, lanes] for k in range(len(pairs))]
            for top in range(0, rows, 8):
                values = [held_ref[i, z, top : top + 8, lanes] for i in range(histories)]
                accs = [acc + values[i] * values[j] for acc, (i, j) in zip(accs, pairs)]
            for k, acc in enumerate(accs):
                acc_ref[k, :, lanes] = acc
        lanes = slice(body_width, width)
        accs = [acc_ref[k, :, body_width:] for k in range(len(pairs))]
        for top in range(0, rows, 16):
            values = [
                jnp.concatenate(
                    [held_ref[i, z, top : top + 8, lanes], held_ref[i, z, top + 8 : top + 16, lanes]],
                    axis=1,
                )
                for i in range(histories)
            ]
            accs = [acc + values[i] * values[j] for acc, (i, j) in zip(accs, pairs)]
        for k, acc in enumerate(accs):
            acc_ref[k, :, body_width:] = acc
        return carry

    lax.fori_loop(0, planes, plane, 0)
    for k in range(len(pairs)):
        grid_part = jnp.sum(acc_ref[k], axis=(0, 1), keepdims=True) / cell_total
        line = jnp.where(lane == k, line + grid_part, line)
    out_ref[...] = jnp.broadcast_to(line, out_ref.shape)


def mixing_weights(line, histories):
    lane = lax.broadcasted_iota(jnp.int32, (1, LANES), 1)
    entry = {}
    for k, (i, j) in enumerate(pair_list(histories)):
        entry[j, i] = jnp.sum(jnp.where(lane == k, line, 0.0), axis=1, keepdims=True)
    factor = {}
    inverse = {}
    work = dict(entry)
    for k in range(histories):
        inverse[k] = 1.0 / work[k, k]
        for i in range(k + 1, histories):
            factor[i, k] = work[i, k] * inverse[k]
        for i in range(k + 1, histories):
            for j in range(k + 1, i + 1):
                work[i, j] = work[i, j] - factor[i, k] * work[j, k]
    solved = [jnp.ones((1, 1), f32) for _ in range(histories)]
    for i in range(histories):
        for k in range(i):
            solved[i] = solved[i] - factor[i, k] * solved[k]
    solved = [value * inverse[i] for i, value in enumerate(solved)]
    for i in reversed(range(histories)):
        for k in range(i + 1, histories):
            solved[i] = solved[i] - factor[k, i] * solved[k]
    total = solved[0]
    for value in solved[1:]:
        total = total + value
    return [value / total for value in solved]


def mix_kernel(
    sums_ref, residual_ref, high_ref, low_ref, out_ref, weights_ref, mixed_high, mixed_low, *, slab_count
):
    histories, planes, rows, _ = residual_ref.shape
    line = jnp.sum(sums_ref[...], axis=0, keepdims=True)
    weights = mixing_weights(line, histories)
    for i, weight in enumerate(weights):
        weights_ref[i : i + 1, :] = jnp.broadcast_to(weight, (1, LANES))
    weights_ref[histories:, :] = jnp.zeros((8 - histories, LANES), f32)
    for z in range(planes):
        mixed = weights[0] * residual_ref[0, z]
        for i in range(1, histories):
            mixed = mixed + weights[i] * residual_ref[i, z]
        high, low = split(mixed)
        filler = jnp.zeros((LANES - rows, mixed.shape[1]), bf16)
        mixed_high[z * LANES : z * LANES + rows, :] = high
        mixed_high[z * LANES + rows : (z + 1) * LANES, :] = filler
        mixed_low[z * LANES : z * LANES + rows, :] = low
        mixed_low[z * LANES + rows : (z + 1) * LANES, :] = filler
    table = (high_ref[...], low_ref[...])
    result = product(table, (mixed_high[...], mixed_low[...]), ((1,), (1,)))
    own_planes = result.shape[0] // slab_count - 1
    part = rows // 2
    lane = lax.broadcasted_iota(jnp.int32, (slab_count, LANES), 1)
    here = (lane >= rows) & (lane < rows + part)
    shared = []
    for shift in (rows, rows - part):
        shared.append(
            [
                jnp.where(
                    here,
                    pltpu.roll(
                        result[own_planes * slab_count :, z * LANES : (z + 1) * LANES], shift, 1
                    ),
                    0.0,
                )
                for z in range(planes)
            ]
        )
    for own in range(own_planes):
        lines = [
            result[own * slab_count : (own + 1) * slab_count, z * LANES : (z + 1) * LANES]
            + shared[own // 2][z]
            for z in range(planes)
        ]
        out_ref[:, own] = jnp.swapaxes(jnp.stack(lines), 0, 1)


def plane_kernel(
    place_ref,
    in_ref,
    zh_ref,
    zl_ref,
    yh_ref,
    yl_ref,
    out_ref,
    made_ref,
    sent,
    *,
    x_length,
    y_length,
    z_length,
    scale,
):
    slab_count, pencil_count, z_local, _ = in_ref.shape
    z_half = z_length // 2
    y_half = y_length // 2
    s_half = slab_count // 2
    fold = pencil_count // 2 * LANES
    in_half = place_ref[1] // 2
    out_half = place_ref[1] % 2

    def gathered(first):
        return jnp.concatenate(
            [
                in_ref[first : first + s_half, q].reshape(z_half, LANES)
                for q in range(pencil_count)
            ],
            axis=1,
        )

    def z_table(kind):
        return (zh_ref[kind], zl_ref[kind])

    def y_table(half, kind):
        return (yh_ref[2 * half + kind], yl_ref[2 * half + kind])

    low, high = gathered(0), gathered(s_half)
    lines = jnp.concatenate(
        [
            product(z_table(0), split(low + high), ((1,), (0,))),
            product(z_table(1), split(low - high), ((1,), (0,))),
        ],
        axis=0,
    )
    folded = [lines[:, :fold] + lines[:, fold:], lines[:, :fold] - lines[:, fold:]]
    row = lax.broadcasted_iota(jnp.int32, (z_length, 1), 0)
    lane = lax.broadcasted_iota(jnp.int32, (1, y_length), 1)
    freq_z = jnp.where(row < z_half, 2 * row, 2 * row - (z_length - 1))
    first_x = place_ref[0] * (pencil_count + 1)
    freq_x = jnp.where(lane < y_half, first_x + place_ref[1], first_x + pencil_count)

    def squared(index, length):
        least = jnp.minimum(index, length - index).astype(f32)
        return least * least

    kept = []
    for kind in range(2):
        spectrum = product(split(folded[kind]), y_table(in_half, kind), ((1,), (0,)))
        freq_y = 2 * jnp.where(lane < y_half, lane, lane - y_half) + kind
        square = squared(freq_z, z_length) + (
            squared(freq_y, y_length) + squared(freq_x, x_length)
        )
        kept.append(spectrum * (square / (square + kerker_wave * kerker_wave) * scale))
    parts = []
    for rows in (slice(0, z_half), slice(z_half, z_length)):
        results = [
            product(split(kept[kind][rows]), y_table(out_half, kind), ((1,), (1,)))
            for kind in range(2)
        ]
        parts.append(split(jnp.concatenate([results[0] + results[1], results[0] - results[1]], axis=1)))
    sends = []
    for q in range(pencil_count):
        for first in (0, s_half):
            here = pl.ds(first, s_half)
            sends.append(
                pltpu.make_async_copy(
                    made_ref.at[here, q], out_ref.at[here, q], sent.at[len(sends)]
                )
            )
    even = product(z_table(0), parts[0], ((1,), (0,)))
    odd = product(z_table(1), parts[1], ((0,), (0,)))
    low, high = even + odd, even - odd
    for q in range(pencil_count):
        columns = slice(q * LANES, (q + 1) * LANES)
        made_ref[:s_half, q] = low[:, columns].reshape(s_half, z_local, LANES)
        sends[2 * q].start()
        made_ref[s_half:, q] = high[:, columns].reshape(s_half, z_local, LANES)
        sends[2 * q + 1].start()
    for send in sends:
        send.wait()


def mean_kernel(
    species_ref, count_ref, weights_ref, density_ref, block_ref, block_residual_ref, out_ref, out_block_ref
):
    step = pl.program_id(0)
    histories = density_ref.shape[0]
    weights = [weights_ref[i : i + 1, 0:1] for i in range(histories)]
    mean = weights[0] * density_ref[0, 0]
    for i in range(1, histories):
        mean = mean + weights[i] * density_ref[i, 0]
    out_ref[0] = mean

    @pl.when(step == 0)
    def _():
        _, slots, entries = block_ref.shape
        mask = block_mask(species_ref, count_ref, slots, entries)
        total = weights[0] * (block_ref[0] + block_mixing * block_residual_ref[0])
        for i in range(1, histories):
            total = total + weights[i] * (block_ref[i] + block_mixing * block_residual_ref[i])
        out_block_ref[...] = jnp.where(mask, total, 0.0)


def x_inverse_kernel(
    in_ref,
    mean_ref,
    high_ref,
    low_ref,
    out_ref,
    field_ref,
    sent,
    *,
    slab_count,
    pencil_count,
    z_local,
):
    rows, x_length = mean_ref.shape
    y_local = rows // z_local
    part = y_local // 2
    table = (high_ref[...], low_ref[...])
    lane = lax.broadcasted_iota(jnp.int32, (slab_count, LANES), 1)
    groups = sent.shape[0]
    group = z_local // groups

    def send(index):
        here = pl.ds(index * group * y_local, group * y_local)
        return pltpu.make_async_copy(field_ref.at[here], out_ref.at[here], sent.at[index])

    blocks = [jnp.swapaxes(in_ref[:, q], 0, 1) for q in range(pencil_count)]
    for index in range(groups):
        lines = []
        for z in range(index * group, (index + 1) * group):
            block = [turned[z] for turned in blocks]
            first = pltpu.roll(block[0] + block[2], LANES - y_local, 1)
            second = pltpu.roll(block[1] + block[3], LANES - y_local + part, 1)
            block.append(jnp.where(lane < part, first, second))
            lines.append(jnp.concatenate(block, axis=0).T[:y_local])
        lines = jnp.concatenate(lines, axis=0)
        field = product(split(lines), table, ((1,), (0,)))
        here = slice(index * group * y_local, (index + 1) * group * y_local)
        field_ref[here, :] = mean_ref[here, :] + field
        send(index).start()
    for index in range(groups):
        send(index).wait()


def whole():
    return pl.BlockSpec(memory_space=pltpu.VMEM)


def scalars():
    return pl.BlockSpec(memory_space=pltpu.SMEM)


def in_hbm(array):
    return pltpu.with_memory_space_constraint(array, pltpu.HBM)


def params(limit):
    return pltpu.CompilerParams(vmem_limit_bytes=limit * MIB)


def body(
    density_history, residual_history, occupancy_history, occupancy_residual, species, slot_count
):
    histories, z_local, y_local, x_length = residual_history.shape
    slab_count = lax.axis_size(SLAB)
    pencil_count = lax.axis_size("pencil")
    devices = slab_count * pencil_count
    y_length = y_local * pencil_count
    z_length = z_local * slab_count
    slots, entries = occupancy_residual.shape[1:]
    kx_local = x_length // slab_count
    rows = devices * z_local
    part = y_local // 2
    cell_total = float(z_length * y_length * x_length)
    x_order = (np.arange(slab_count)[None, :] * kx_local + np.arange(kx_local)[:, None]).reshape(-1)
    x_table = hartley(x_order, np.arange(x_length), x_length)
    y_tables = []
    for half in range(2):
        for kind in range(2):
            freq = 2 * np.arange(y_length // 2) + kind
            terms = [np.zeros((pencil_count // 2, LANES, 2, y_length // 2), bf16) for _ in range(2)]
            for q in range(pencil_count // 2):
                point = q * y_local + np.arange(y_local)
                whole_terms = hartley(point, freq, y_length)
                part_terms = hartley(point[half * part : (half + 1) * part], freq, y_length)
                for term, own, some in zip(terms, whole_terms, part_terms):
                    term[q, :y_local, 0] = own
                    term[q, y_local : y_local + part, 1] = some
            y_tables.append([term.reshape(-1, y_length) for term in terms])
    y_table = [np.stack(terms) for terms in zip(*y_tables)]
    z_half = np.arange(z_length // 2)
    z_table = [
        np.stack(terms)
        for terms in zip(
            hartley(2 * z_half, z_half, z_length),
            hartley(2 * z_half + 1, z_half, z_length),
        )
    ]
    place = jnp.stack([lax.axis_index(SLAB), lax.axis_index("pencil")]).astype(jnp.int32)
    place, species = lax.optimization_barrier((place, species))

    sums, held = pl.pallas_call(
        functools.partial(
            gram_kernel, cell_total=cell_total, block_total=100.0 * slots * devices
        ),
        in_specs=[scalars(), scalars(), pl.BlockSpec(memory_space=pltpu.HBM), whole()],
        out_specs=[whole(), whole()],
        out_shape=[
            jax.ShapeDtypeStruct((devices, LANES), f32),
            jax.ShapeDtypeStruct(residual_history.shape, f32),
        ],
        scratch_shapes=[
            pltpu.VMEM((len(pair_list(histories)), 8, -(-x_length // LANES) * LANES), f32),
            pltpu.SemaphoreType.DMA((z_local,)),
        ],
        compiler_params=params(16),
        name="gram",
    )(in_hbm(species), slot_count, in_hbm(residual_history), in_hbm(occupancy_residual))

    def exchange(array):
        return lax.all_to_all(
            array.reshape(devices, -1, LANES), SLAB_PENCIL, split_axis=0, concat_axis=0, tiled=True
        )

    sums = exchange(sums).reshape(devices, LANES)
    packed, weights = pl.pallas_call(
        functools.partial(mix_kernel, slab_count=slab_count),
        in_specs=[whole()] * 4,
        out_specs=[whole(), whole()],
        out_shape=[
            jax.ShapeDtypeStruct((slab_count, pencil_count, z_local, LANES), f32),
            jax.ShapeDtypeStruct((8, LANES), f32),
        ],
        scratch_shapes=[
            pltpu.VMEM((z_local * LANES, x_length), bf16),
            pltpu.VMEM((z_local * LANES, x_length), bf16),
        ],
        compiler_params=params(24),
        name="mix",
    )(sums, held, *x_table)
    moved = exchange(packed).reshape(slab_count, pencil_count, z_local, LANES)
    plane_in = pl.BlockSpec((histories, 1, y_local, x_length), lambda z: (0, z, 0, 0))
    mean, new_occupancy = pl.pallas_call(
        mean_kernel,
        grid=(z_local,),
        in_specs=[scalars(), scalars(), whole(), plane_in, whole(), whole()],
        out_specs=[
            pl.BlockSpec((1, y_local, x_length), lambda z: (z, 0, 0)),
            whole(),
        ],
        out_shape=[
            jax.ShapeDtypeStruct((z_local, y_local, x_length), f32),
            jax.ShapeDtypeStruct((slots, entries), f32),
        ],
        compiler_params=params(16),
        name="mean",
    )(species, slot_count, weights, density_history, occupancy_history, occupancy_residual)
    packed = pl.pallas_call(
        functools.partial(
            plane_kernel,
            x_length=x_length,
            y_length=y_length,
            z_length=z_length,
            scale=grid_mixing / cell_total,
        ),
        in_specs=[scalars()] + [whole()] * 5,
        out_specs=pl.BlockSpec(memory_space=pltpu.HBM),
        out_shape=jax.ShapeDtypeStruct((slab_count, pencil_count, z_local, LANES), f32),
        scratch_shapes=[
            pltpu.VMEM((slab_count, pencil_count, z_local, LANES), f32),
            pltpu.SemaphoreType.DMA((2 * pencil_count,)),
        ],
        compiler_params=params(32),
        name="plane",
    )(place, moved, *z_table, *y_table)
    moved = exchange(packed).reshape(slab_count, pencil_count, z_local, LANES)
    new_density = pl.pallas_call(
        functools.partial(
            x_inverse_kernel, slab_count=slab_count, pencil_count=pencil_count, z_local=z_local
        ),
        in_specs=[whole()] * 4,
        out_specs=pl.BlockSpec(memory_space=pltpu.HBM),
        out_shape=jax.ShapeDtypeStruct((z_local * y_local, x_length), f32),
        scratch_shapes=[
            pltpu.VMEM((z_local * y_local, x_length), f32),
            pltpu.SemaphoreType.DMA((2,)),
        ],
        compiler_params=params(24),
        name="x_inverse",
    )(moved, mean.reshape(z_local * y_local, x_length), *x_table)
    return (new_density.reshape(z_local, y_local, x_length), new_occupancy)


def solution(mesh):
    torus = Mesh(
        mesh.devices.reshape(8, 4, 2, mesh.shape["pencil"]),
        ("slab_0", "slab_1", "slab_2", "pencil"),
    )
    placed = (
        P(None, SLAB, "pencil", None),
        P(None, SLAB, "pencil", None),
        P(None, SLAB_PENCIL, None),
        P(None, SLAB_PENCIL, None),
        P(SLAB_PENCIL),
        P(SLAB_PENCIL),
    )
    return jax.shard_map(
        body,
        mesh=torus,
        in_specs=placed,
        out_specs=(P(SLAB, "pencil", None), P(SLAB_PENCIL, None)),
        check_vma=False,
    )
```
